32 devices in a mesh: dp: 8 (over z, x), section: 4 (over y, core).
Axes of the slice: x: 2, y: 2, z: 4, core: 2. Of those that a mesh axis runs over, the one named last changes fastest.
Arguments:
- hidden_in: bfloat16 [4, 4, 8, 96, 2048], P('section', None, 'dp'), may hold values from -170 to 170
- queries: bfloat16 [4, 4, 8, 96, 2048], P('section', None, 'dp'), may hold values from -96 to 96
- keys: bfloat16 [4, 4, 8, 96, 2048], P('section', None, 'dp'), may hold values from -6 to 6
- values: bfloat16 [4, 4, 8, 96, 2048], P('section', None, 'dp'), may hold values from -6 to 6
- cotangent: bfloat16 [4, 8, 96, 2048], P(None, 'dp'), may hold values from -6 to 6
- norm_gain: float32 [4, 2048], P('section'), may hold values from 0.1 to 1.9
- w_query: bfloat16 [4, 2048, 2048], P('section', 'dp'), may hold values from -0.125 to 0.125
- w_key: bfloat16 [4, 2048, 2048], P('section', 'dp'), may hold values from -0.125 to 0.125
- w_value: bfloat16 [4, 2048, 2048], P('section', 'dp'), may hold values from -0.125 to 0.125
- down_q: bfloat16 [4, 16, 2048], P('section'), may hold values from -0.125 to 0.125
- up_q: bfloat16 [4, 16, 2048], P('section'), may hold values from -0.75 to 0.75
- down_v: bfloat16 [4, 16, 2048], P('section'), may hold values from -0.125 to 0.125
- up_v: bfloat16 [4, 16, 2048], P('section'), may hold values from -0.75 to 0.75
Outputs:
- input_grad: bfloat16 [4, 4, 8, 96, 2048], P('section', None, 'dp')
- grad_down_q: float32 [4, 16, 2048], P('section')
- grad_up_q: float32 [4, 16, 2048], P('section')
- grad_down_v: float32 [4, 16, 2048], P('section')
- grad_up_v: float32 [4, 16, 2048], P('section')
The draws below stay inside these ranges and needn't reach their ends.
All inputs are finite; a program needn't handle non-finite values.
Results may differ from the reference program's by a relative error of at most 0.025.
Values may be sent and summed in bfloat16 or wider, within the bound.
A program may use at most 128 MiB of HBM per device.

```python
import jax
import jax.numpy as jnp
from jax import lax

HEADS = 16
HEAD_DIM = 128
D = 2048
RANK = 16
MICRO = 4
SEQ = 96
LAYERS = 4
BATCH = 8


def attention_pair(key):
    full_shape = (LAYERS, MICRO, BATCH, SEQ, HEADS, HEAD_DIM)
    first = jax.random.normal(jax.random.fold_in(key, 11), full_shape, jnp.float32)
    second = jax.random.normal(jax.random.fold_in(key, 23), full_shape, jnp.float32)
    query = jnp.clip(first, -6.0, 6.0)
    keyed = jnp.clip(second, -6.0, 6.0)
    final_shape = (LAYERS, MICRO, BATCH, SEQ, HEADS * HEAD_DIM)
    return (query.reshape(final_shape), keyed.reshape(final_shape))


def draw_queries(key, part):
    return attention_pair(key)[0].astype(jnp.bfloat16)


def draw_keys(key, part):
    return attention_pair(key)[1].astype(jnp.bfloat16)


def draw_hidden_in(key, part):
    full_shape = (LAYERS, MICRO, BATCH, SEQ, D)
    base = jnp.clip(jax.random.normal(jax.random.fold_in(key, 41), full_shape, jnp.float32), -6.0, 6.0)
    return base.astype(jnp.bfloat16)


def level_of(stream_key, dims, shards, low, high):
    gain, own = 1.0, jax.random.fold_in(stream_key, 6)
    for axis_at, blocks in shards:
        steps = jnp.exp(jax.random.uniform(jax.random.fold_in(own, axis_at), (blocks,), jnp.float32, low / len(shards), high / len(shards)))
        gain = gain * jnp.repeat(steps, dims[axis_at] // blocks).reshape([-1 if axis == axis_at else 1 for axis in range(len(dims))])
    return gain


def normal_values(rng, shape, deviation, bound, cuts=(), kind=jnp.bfloat16):
    gain = level_of(rng, shape, cuts, -0.22, 0.18) if cuts else 1.0
    drawn = jax.random.normal(rng, shape, jnp.float32) * deviation * gain
    return jnp.minimum(jnp.maximum(drawn, -bound), bound).astype(kind)


def setup_inputs(seed: int = 0) -> dict:
    splits = jax.random.split(jax.random.key(seed), 14)
    hidden_in = draw_hidden_in(jax.random.fold_in(splits[13], 71), 0)
    queries = draw_queries(jax.random.fold_in(splits[13], 71), 0)
    keys = draw_keys(jax.random.fold_in(splits[13], 71), 0)
    values = normal_values(splits[3], (LAYERS, MICRO, BATCH, SEQ, D), 1.0, 6.0, ((0, 4), (2, 8)))
    cotangent = normal_values(splits[4], (MICRO, BATCH, SEQ, D), 1.0, 6.0, ((1, 8),))
    norm_gain = jnp.clip(1.0 + 0.18 * jax.random.normal(splits[5], (LAYERS, D), jnp.float32), 0.1, 1.9)
    w_query = normal_values(splits[6], (LAYERS, D, D), D ** -0.5, 0.125, ((0, 4), (1, 8)))
    w_key = normal_values(splits[7], (LAYERS, D, D), D ** -0.5, 0.125, ((0, 4), (1, 8)))
    w_value = normal_values(splits[8], (LAYERS, D, D), D ** -0.5, 0.125, ((0, 4), (1, 8)))
    down_q = normal_values(splits[9], (LAYERS, RANK, D), D ** -0.5, 0.125, ((0, 4),))
    up_q = normal_values(splits[10], (LAYERS, RANK, D), (4 * RANK) ** -0.5, 0.75, ((0, 4),))
    down_v = normal_values(splits[11], (LAYERS, RANK, D), D ** -0.5, 0.125, ((0, 4),))
    up_v = normal_values(splits[12], (LAYERS, RANK, D), (4 * RANK) ** -0.5, 0.75, ((0, 4),))
    return {"hidden_in": hidden_in, "queries": queries, "keys": keys, "values": values, "cotangent": cotangent, "norm_gain": norm_gain, "w_query": w_query, "w_key": w_key, "w_value": w_value, "down_q": down_q, "up_q": up_q, "down_v": down_v, "up_v": up_v}


adapter_scale = 2.0
norm_eps = 1e-05

def input_backward(hidden, query, keyed, valued, out_grad, gain_row, frozen, adapter_weights):
    count, positions, features = hidden.shape
    head_count = features // HEAD_DIM
    scale = HEAD_DIM ** (-0.5)
    floated = hidden.astype(jnp.float32)
    inverse = lax.rsqrt(lax.optimization_barrier(jnp.mean(floated * floated, axis=-1, keepdims=True)) + norm_eps)
    normed = (floated * inverse * gain_row).astype(jnp.bfloat16)
    split = (count, positions, head_count, HEAD_DIM)
    query_heads = query.astype(jnp.float32).reshape(split)
    key_heads = keyed.astype(jnp.float32).reshape(split)
    value_heads = valued.astype(jnp.float32).reshape(split)
    grad_heads = out_grad.astype(jnp.float32).reshape(split)
    scores = jnp.einsum('nqhd,nkhd->nhqk', query_heads, key_heads) * scale
    causal = lax.broadcasted_iota(jnp.int32, (positions, positions), 1) <= lax.broadcasted_iota(jnp.int32, (positions, positions), 0)
    scores = jnp.where(causal, scores, -1e+30)
    attend = jax.nn.softmax(scores, axis=-1)
    attend_low = lax.optimization_barrier(attend.astype(jnp.bfloat16)).astype(jnp.float32)
    attend_grad = jnp.einsum('nqhd,nkhd->nhqk', grad_heads, value_heads)
    value_grad = jnp.einsum('nhqk,nqhd->nkhd', attend_low, grad_heads).astype(jnp.bfloat16)
    row_total = lax.optimization_barrier(jnp.sum(attend * attend_grad, axis=-1, keepdims=True))
    score_grad = (attend * (attend_grad - row_total) * scale).astype(jnp.bfloat16)
    score_wide = lax.optimization_barrier(score_grad).astype(jnp.float32)
    query_grad = jnp.einsum('nhqk,nkhd->nqhd', score_wide, key_heads).astype(jnp.bfloat16)
    key_grad = jnp.einsum('nhqk,nqhd->nkhd', score_wide, query_heads).astype(jnp.bfloat16)
    rows = count * positions
    flattened_query = query_grad.reshape(rows, features)
    key_flat = key_grad.reshape(rows, features)
    flattened_value = value_grad.reshape(rows, features)
    contract_matrices = (((1,), (1,)), ((), ()))
    normed_grad = lax.dot_general(flattened_query, frozen[0], contract_matrices, preferred_element_type=jnp.float32)
    normed_grad = normed_grad + lax.dot_general(key_flat, frozen[1], contract_matrices, preferred_element_type=jnp.float32)
    normed_grad = normed_grad + lax.dot_general(flattened_value, frozen[2], contract_matrices, preferred_element_type=jnp.float32)
    query_low_rank = (adapter_scale * lax.dot_general(flattened_query, adapter_weights[1], contract_matrices, preferred_element_type=jnp.float32)).astype(jnp.bfloat16)
    value_low_rank = (adapter_scale * lax.dot_general(flattened_value, adapter_weights[3], contract_matrices, preferred_element_type=jnp.float32)).astype(jnp.bfloat16)
    normed_grad = normed_grad + jnp.dot(query_low_rank, adapter_weights[0], preferred_element_type=jnp.float32)
    normed_grad = normed_grad + jnp.dot(value_low_rank, adapter_weights[2], preferred_element_type=jnp.float32)
    scaled_grad = (gain_row * normed_grad).reshape(count, positions, features)
    correction = lax.optimization_barrier(jnp.mean(floated * scaled_grad, axis=-1, keepdims=True))
    input_grad = (out_grad.astype(jnp.float32) + inverse * scaled_grad - floated * inverse ** 3 * correction).astype(jnp.bfloat16)
    saved = (normed.reshape(rows, features), flattened_query, flattened_value, query_low_rank, value_low_rank)
    return (input_grad, saved)

def adapter_grads(normed, flattened_query, flattened_value, query_low_rank, value_low_rank, down_query, down_value):
    contract_matrices = (((1,), (1,)), ((), ()))
    across_replicas_total = (((0,), (0,)), ((), ()))
    normalized_query = lax.dot_general(normed, down_query, contract_matrices, preferred_element_type=jnp.float32).astype(jnp.bfloat16)
    normalized_value = lax.dot_general(normed, down_value, contract_matrices, preferred_element_type=jnp.float32).astype(jnp.bfloat16)
    grad_dq = lax.dot_general(query_low_rank, normed, across_replicas_total, preferred_element_type=jnp.float32)
    query_up_gradient = adapter_scale * lax.dot_general(normalized_query, flattened_query, across_replicas_total, preferred_element_type=jnp.float32)
    grad_dv = lax.dot_general(value_low_rank, normed, across_replicas_total, preferred_element_type=jnp.float32)
    value_up_gradient = adapter_scale * lax.dot_general(normalized_value, flattened_value, across_replicas_total, preferred_element_type=jnp.float32)
    return (grad_dq, query_up_gradient, grad_dv, value_up_gradient)

def reference(hidden_in, queries, keys, values, cotangent, norm_gain, w_query, w_key, w_value, down_q, up_q, down_v, up_v):
    count = MICRO * BATCH
    out_grad = cotangent.reshape(count, SEQ, D)
    input_list = []
    grad_lists = ([], [], [], [])
    for current in reversed(range(LAYERS)):
        frozen = (w_query[current], w_key[current], w_value[current])
        adapter_weights = (down_q[current], up_q[current], down_v[current], up_v[current])
        input_grad, saved = input_backward(hidden_in[current].reshape(count, SEQ, D), queries[current].reshape(count, SEQ, D), keys[current].reshape(count, SEQ, D), values[current].reshape(count, SEQ, D), out_grad, norm_gain[current], frozen, adapter_weights)
        totals = adapter_grads(*saved, adapter_weights[0], adapter_weights[2])
        input_list.append(input_grad)
        for target, total in zip(grad_lists, totals):
            target.append(total)
        out_grad = input_grad
    ordered = input_list[::-1]
    scale = (MICRO * BATCH * SEQ) ** (-0.5)
    stacked = [jnp.stack(target[::-1]) * scale for target in grad_lists]
    input_all = jnp.stack(ordered).reshape(LAYERS, MICRO, BATCH, SEQ, D)
    return (input_all, stacked[0], stacked[1], stacked[2], stacked[3])
```

```python
import functools

import jax
import jax.numpy as jnp
from jax import lax
from jax.experimental import pallas as pl
from jax.experimental.pallas import tpu as pltpu
from jax.sharding import PartitionSpec as P

HEAD_DIM = 128
adapter_scale = 2.0
norm_eps = 1e-05
NN = (((1,), (0,)), ((), ()))
NT = (((1,), (1,)), ((), ()))
TN = (((0,), (0,)), ((), ()))
F32 = jnp.float32
BF16 = jnp.bfloat16
MESH = pl.DeviceIdType.MESH
PAIR = 2


def dot(a, b, dims):
    return lax.dot_general(a, b, dims, preferred_element_type=F32)


def drain(ref, sem):
    pltpu.make_async_copy(ref, ref, sem).wait()


def remote(src, dst, send, recv, device):
    return pltpu.make_async_remote_copy(
        src_ref=src, dst_ref=dst, send_sem=send, recv_sem=recv, device_id=device, device_id_type=MESH
    )


def flip(value, k, size):
    if size & (size - 1):
        return lax.rem(value + k, size)
    out, bit = 0, 1
    while bit < size:
        out = out + bit * lax.rem(lax.div(value, bit) + (k // bit) % 2, 2)
        bit *= 2
    return out


def kernel(
    n_dp, layers, micro, seq, features, rank, rows_w, total_scale,
    hid, que, key, val, cot, gain, wq, wk, wv, dq, uq, dv, uv,
    out_ig, out_g,
    wbuf, act, hown, og, ab, nrm, ad, gn, st, st_own, lows, lowr, lowt,
    cs, crecv, ctmp, cown, xs, xrecv, sc, rs_own, rsr, crow, gr, gf,
    w_s, w_r, q_s, q_r, h_s, h_r, ad_s, ad_r, gn_s, gn_r, cot_s, cot_r, hown_sem, st_s, st_r,
    z_s, z_r, rel_s, lo_s, lo_r, d_s, d_r, x_s, x_r, rs_s, rs_r, o_s, o_r, g_s, g_r, f_s, f_r,
):
    sections = layers
    planes = n_dp // PAIR
    cols = PAIR * sections
    chips = cols // 2
    hw = features // cols
    heads = hw // HEAD_DIM
    seqs = PAIR * micro
    rows = seqs * seq
    block = PAIR * rows_w
    dp, s = lax.axis_index("dp"), lax.axis_index("section")
    a, x = lax.div(dp, PAIR), lax.rem(dp, PAIR)
    f = x * sections + s
    c = lax.rem(f, 2)
    chip = lax.div(f, 2)

    def device(j):
        return (PAIR * a + lax.div(j, sections), lax.rem(j, sections))

    others = [flip(f, k, cols) for k in range(1, cols)]

    def col_of(j):
        return pl.ds(pl.multiple_of(j * hw, hw), hw)

    barrier = pltpu.get_barrier_semaphore()
    for j in others:
        pl.semaphore_signal(barrier, inc=1, device_id=device(j), device_id_type=MESH)
    for k in range(1, planes):
        pl.semaphore_signal(
            barrier, inc=1, device_id=(PAIR * lax.rem(a + k, planes) + x, s), device_id_type=MESH
        )
    pl.semaphore_wait(barrier, cols - 1 + planes - 1)

    own_hidden = pltpu.make_async_copy(hid.at[0, :, 0], hown, hown_sem)
    own_hidden.start()
    for k in range(sections):
        s2 = s if k == 0 else flip(s, k, sections)
        cut = col_of(x * sections + s2)
        for i, ref in enumerate((dq, dv, uq, uv)):
            src, dst = ref.at[0, :, cut], ad.at[s, pl.ds(i * rank, rank), :]
            if k == 0:
                pltpu.make_async_copy(src, dst, ad_r.at[s]).start()
            else:
                remote(src, dst, ad_s.at[k], ad_r.at[s], (dp, s2)).start()
        src, dst = gain.at[:, cut], gn.at[s]
        if k == 0:
            pltpu.make_async_copy(src, dst, gn_r.at[s]).start()
        else:
            remote(src, dst, gn_s.at[k], gn_r.at[s], (dp, s2)).start()
    mirror = (PAIR * a + 1 - x, s)
    remote(cot.at[:, 0, :, col_of((1 - x) * sections + s)], og.at[x], cot_s.at[0], cot_r.at[0], mirror).start()
    pltpu.make_async_copy(cot.at[:, 0, :, col_of(f)], og.at[x], cot_r.at[1]).start()

    def send_big():
        def weights(j):
            for i, ref in enumerate((wq, wk, wv)):
                yield ref.at[0, :, col_of(j)], wbuf.at[s, a, pl.ds(x * rows_w, rows_w), pl.ds(i * hw, hw)]

        def saved(j):
            for i, ref in enumerate((que, key, val)):
                yield ref.at[0, :, 0, :, col_of(j)], act.at[s, x, i]

        def inputs(j):
            yield hid.at[0, :, 0, :, col_of(j)], act.at[s, x, 3]

        for group, send, recv in ((weights, w_s, w_r), (saved, q_s, q_r), (inputs, h_s, h_r)):
            for k, j in enumerate(others):
                for src, dst in group(j):
                    remote(src, dst, send.at[k], recv.at[f], device(j)).start()
            for src, dst in group(f):
                pltpu.make_async_copy(src, dst, recv.at[f]).start()

    early = lax.rem(layers - 1 - s, 2) == 0
    pl.when(early)(send_big)

    eye = lax.broadcasted_iota(jnp.int32, (seq, 128), 0) == lax.broadcasted_iota(jnp.int32, (seq, 128), 1)

    def to_row(column):
        return jnp.sum(jnp.where(eye, column, 0.0), axis=0, keepdims=True)

    def to_column(row):
        return jnp.sum(jnp.where(eye, row, 0.0), axis=1, keepdims=True)

    own_hidden.wait()

    def inverse_of(m, carry):
        floated = hown[m].astype(F32)
        inverse = lax.rsqrt(jnp.mean(floated * floated, axis=-1, keepdims=True) + norm_eps)
        st_own[pl.ds(m, 1), :] = to_row(inverse)
        return carry

    lax.fori_loop(0, micro, inverse_of, 0)
    st[f] = st_own[...]
    for k, j in enumerate(others):
        remote(st_own, st.at[f], st_s.at[k], st_r.at[f], device(j)).start()

    def z_own(l):
        for xx in range(PAIR):
            drain(wbuf.at[l, a, pl.ds(xx * rows_w, rows_w), :], w_r.at[xx * sections + l])
        for i, d in enumerate((2, -2, 1, -1)):
            if abs(d) >= planes:
                continue

            @pl.when((a + d >= 0) & (a + d < planes))
            def _():
                remote(
                    wbuf.at[l, a], wbuf.at[l, a], z_s.at[l, i], z_r.at[l, a], (PAIR * (a + d) + x, s)
                ).start()

    def passed_on(l, b, todo):
        for direction in (1, -1):

            @pl.when(((a - b) * direction >= 2) & (a + direction >= 0) & (a + direction < planes))
            def _():
                todo(
                    remote(
                        wbuf.at[l, b], wbuf.at[l, b], rel_s.at[l, b], z_r.at[l, b],
                        (PAIR * (a + direction) + x, s),
                    )
                )

    def take(l, b):
        drain(wbuf.at[l, b], z_r.at[l, b])
        passed_on(l, b, lambda copy: copy.start())

    scale = HEAD_DIM ** (-0.5)
    causal = lax.broadcasted_iota(jnp.int32, (seq, seq), 1) <= lax.broadcasted_iota(jnp.int32, (seq, seq), 0)
    z_own(layers - 1)

    def finish_grads(l):
        for k in range(1, planes):
            b = lax.rem(a + k, planes)
            drain(gr.at[l, b], g_r.at[l, b])
        total = gr[l, 0].astype(F32)
        for b in range(1, planes):
            total = total + gr[l, b].astype(F32)
        gf[l] = total * total_scale
        for xx in range(PAIR):
            mine = (x == xx) & (s == l)

            @pl.when(mine)
            def _():
                pltpu.make_async_copy(gf.at[l], out_g.at[:, col_of(f)], f_s.at[l, xx]).start()

            @pl.when(jnp.logical_not(mine))
            def _():
                remote(
                    gf.at[l], out_g.at[:, col_of(f)], f_s.at[l, xx], f_r.at[f], (PAIR * a + xx, l)
                ).start()

    def layer(i, carry):
        l = layers - 1 - i
        for xx in range(PAIR):
            drain(act.at[l, xx, pl.ds(0, 3)], q_r.at[xx * sections + l])

        @pl.when(i == 0)
        def _():
            pl.when(jnp.logical_not(early))(send_big)
            drain(og.at[0], cot_r.at[0])
            drain(og.at[0], cot_r.at[1])

        def attention(n, carry):
            xx, m = lax.div(n, micro), lax.rem(n, micro)
            for h in range(heads):
                at = pl.ds(h * HEAD_DIM, HEAD_DIM)
                q, k, v = (act[l, xx, t, m, :, at] for t in range(3))
                g = og[xx, m, :, at]
                scores = jnp.where(causal, dot(q, k, NT) * scale, -1e30)
                grown = jnp.exp(scores - jnp.max(scores, axis=-1, keepdims=True))
                attend = grown / jnp.sum(grown, axis=-1, keepdims=True)
                attend_grad = dot(g, v, NT)
                value_grad = dot(attend.astype(BF16), g, TN)
                row_total = jnp.sum(attend * attend_grad, axis=-1, keepdims=True)
                score_grad = (attend * (attend_grad - row_total) * scale).astype(BF16)
                ab[n, :, at] = dot(score_grad, k, NN).astype(BF16)
                ab[n, :, pl.ds(hw + h * HEAD_DIM, HEAD_DIM)] = dot(score_grad, q, TN).astype(BF16)
                ab[n, :, pl.ds(2 * hw + h * HEAD_DIM, HEAD_DIM)] = value_grad.astype(BF16)
            return carry

        lax.fori_loop(0, seqs, attention, 0)

        for xx in range(PAIR):
            j = xx * sections + l
            drain(act.at[l, xx, 3], h_r.at[j])

            @pl.when(j != f)
            def _():
                drain(st.at[j], st_r.at[j])

        drain(ad.at[l], ad_r.at[l])
        drain(gn.at[l], gn_r.at[l])
        gains = gn[l]

        def normalise(n, carry):
            xx, m = lax.div(n, micro), lax.rem(n, micro)
            inverse = to_column(st[xx * sections + l, pl.ds(m, 1), :])
            nrm[n] = (act[l, xx, 3, m].astype(F32) * inverse * gains).astype(BF16)
            return carry

        lax.fori_loop(0, seqs, normalise, 0)

        def flat(value):
            return value.reshape(rows, value.shape[-1])

        normed = flat(nrm[...])
        down = ad[l, : 2 * rank]
        lows[:rank] = (adapter_scale * dot(ad[l, 2 * rank : 3 * rank], flat(ab[:, :, :hw]), NT)).astype(BF16)
        lows[rank : 2 * rank] = (
            adapter_scale * dot(ad[l, 3 * rank :], flat(ab[:, :, 2 * hw :]), NT)
        ).astype(BF16)
        lows[2 * rank :] = dot(down, normed, NT).astype(BF16)
        for k, j in enumerate(others):
            remote(lows, lowr.at[f], lo_s.at[k], lo_r.at[f], device(j)).start()

        @pl.when(i > 0)
        def _():
            finish_grads(l + 1)

        def next_own():
            @pl.when(l > 0)
            def _():
                z_own(l - 1)

        def half(p, cc):
            start = (2 * p + cc) * hw
            w = wbuf[l, lax.div(start, block), pl.ds(pl.multiple_of(lax.rem(start, block), hw), hw), :]
            return dot(flat(ab[...]), w, NT).reshape(seqs, seq, hw)

        partner = flip(f, 1, cols)

        def pair(p):
            cs[p] = half(p, 1 - c).astype(BF16)
            to_partner = remote(cs.at[p], crecv.at[p], d_s.at[p], d_r.at[p], device(partner))
            to_partner.start()
            ctmp[...] = half(p, c)
            to_partner.wait_recv()

            @pl.when(p == chip)
            def _():
                cown[...] = ctmp[...] + crecv[p].astype(F32)

            @pl.when(p != chip)
            def _():
                xs[p] = (ctmp[...] + crecv[p].astype(F32)).astype(BF16)
                remote(xs.at[p], xrecv.at[chip], x_s.at[p], x_r.at[chip], device(2 * p + c)).start()

        if planes == 4 and chips == 4:
            upper = lax.div(a, 2)
            near = a + upper * (3 - 2 * a)
            for k in range(4):
                lower = lax.rem(near + k, 2) if k < 2 else k
                p = lower + upper * (3 - 2 * lower)
                relays = (a == 1) | (a == 2)
                if k == 3:
                    pl.when(jnp.logical_not(relays))(next_own)
                if k > 0:
                    take(l, p)
                if k == 3:
                    pl.when(relays)(next_own)
                pair(p)
        else:
            for d in range(1, planes):
                for b in (a - d, a + d):

                    @pl.when((b >= 0) & (b < planes))
                    def _():
                        take(l, b)

            next_own()
            for k in range(chips):
                pair(lax.rem(chip + k, chips))

        total = lows[...].astype(F32)
        for j in others:
            drain(lowr.at[j], lo_r.at[j])
        for j in others:
            total = total + lowr[j].astype(F32)
        lowt[...] = total.astype(BF16)
        sc[...] = dot(lowt[: 2 * rank], down, TN).reshape(seqs, seq, hw)
        for k in range(1, chips):
            j = flip(chip, k, chips)
            drain(xrecv.at[j], x_r.at[j])

        def gather_up(n, carry):
            xx, m = lax.div(n, micro), lax.rem(n, micro)
            value = sc[n] + cown[n]
            for k in range(1, chips):
                value = value + xrecv[flip(chip, k, chips), n].astype(F32)
            value = gains * value
            sc[n] = value
            rs_own[pl.ds(n, 1), :] = to_row(
                jnp.sum(act[l, xx, 3, m].astype(F32) * value, axis=-1, keepdims=True)
            )
            return carry

        lax.fori_loop(0, seqs, gather_up, 0)
        for k, j in enumerate(others):
            remote(rs_own, rsr.at[f], rs_s.at[k], rs_r.at[f], device(j)).start()
        for j in others:
            drain(rsr.at[j], rs_r.at[j])
        correction = rs_own[...]
        for j in others:
            correction = correction + rsr[j]
        crow[...] = correction * (1.0 / features)

        @pl.when(i > 0)
        def _():
            for xx in range(PAIR):
                drain(og.at[xx], o_s.at[xx])

        def settle(n, carry):
            xx, m = lax.div(n, micro), lax.rem(n, micro)
            inverse = to_column(st[xx * sections + l, pl.ds(m, 1), :])
            corrected = to_column(crow[pl.ds(n, 1), :])
            hidden = act[l, xx, 3, m].astype(F32)
            og[xx, m] = (
                og[xx, m].astype(F32) + inverse * sc[n] - hidden * (inverse * inverse * inverse * corrected)
            ).astype(BF16)
            return carry

        lax.fori_loop(0, seqs, settle, 0)
        for xx in range(PAIR):
            mine = (x == xx) & (s == l)

            @pl.when(mine)
            def _():
                pltpu.make_async_copy(og.at[xx], out_ig.at[0, :, 0, :, col_of(f)], o_s.at[xx]).start()

            @pl.when(jnp.logical_not(mine))
            def _():
                remote(
                    og.at[xx], out_ig.at[0, :, 0, :, col_of(f)], o_s.at[xx], o_r.at[f], (PAIR * a + xx, l)
                ).start()

        gr[l, a, : 2 * rank] = dot(lowt[: 2 * rank], normed, NN).astype(BF16)
        gr[l, a, 2 * rank : 3 * rank] = (
            adapter_scale * dot(lowt[2 * rank : 3 * rank], flat(ab[:, :, :hw]), NN)
        ).astype(BF16)
        gr[l, a, 3 * rank :] = (adapter_scale * dot(lowt[3 * rank :], flat(ab[:, :, 2 * hw :]), NN)).astype(BF16)
        for k in range(1, planes):
            remote(
                gr.at[l, a], gr.at[l, a], g_s.at[l, k], g_r.at[l, a], (PAIR * lax.rem(a + k, planes) + x, s)
            ).start()

        for k in range(cols - 1):
            drain(lows, lo_s.at[k])
            drain(rs_own, rs_s.at[k])
        for p in range(chips):
            drain(cs.at[p], d_s.at[p])
        for k in range(1, chips):
            j = flip(chip, k, chips)
            drain(xs.at[j], x_s.at[j])
        return carry

    lax.fori_loop(0, layers, layer, 0)
    finish_grads(0)

    for xx in range(PAIR):
        drain(og.at[xx], o_s.at[xx])
    for j in others:
        drain(out_ig.at[0, :, 0, :, col_of(j)], o_r.at[j])
        drain(out_g.at[:, col_of(j)], f_r.at[j])
    for k in range(1, sections):
        drain(ad.at[0], ad_s.at[k])
        drain(gn.at[0], gn_s.at[k])
    drain(og.at[0], cot_s.at[0])
    for k in range(cols - 1):
        drain(wbuf.at[0, 0, pl.ds(0, rows_w), :], w_s.at[k])
        drain(act.at[0, 0, pl.ds(0, 3)], q_s.at[k])
        drain(act.at[0, 0, 3], h_s.at[k])
        drain(st_own, st_s.at[k])

    def sent(l, carry):
        for i, d in enumerate((2, -2, 1, -1)):
            if abs(d) >= planes:
                continue

            @pl.when((a + d >= 0) & (a + d < planes))
            def _():
                drain(wbuf.at[l, a], z_s.at[l, i])

        for d in range(2, planes):
            for b in (a - d, a + d):

                @pl.when((b >= 0) & (b < planes))
                def _():
                    passed_on(l, b, lambda copy: copy.wait_send())

        for k in range(1, planes):
            drain(gr.at[l, a], g_s.at[l, k])
        for xx in range(PAIR):
            drain(gf.at[l], f_s.at[l, xx])
        return carry

    lax.fori_loop(0, layers, sent, 0)


def on_device(n_dp, layers, *args):
    hidden, cot, w, down = args[0], args[4], args[6], args[9]
    micro, seq, features = cot.shape[0], cot.shape[2], cot.shape[3]
    batch = cot.shape[1] * n_dp
    rank, rows_w = down.shape[1], w.shape[1]
    planes, cols = n_dp // PAIR, PAIR * layers
    chips, hw, seqs = cols // 2, features // cols, PAIR * micro
    rows = seqs * seq
    pad = -(-micro // 8) * 8
    pads = -(-seqs // 8) * 8
    dma = pltpu.SemaphoreType.DMA
    vm = pltpu.VMEM
    scratch = [
        vm((layers, planes, PAIR * rows_w, 3 * hw), BF16),
        vm((layers, PAIR, 4, micro, seq, hw), BF16),
        vm((micro, seq, features), BF16),
        vm((PAIR, micro, seq, hw), BF16),
        vm((seqs, seq, 3 * hw), BF16),
        vm((seqs, seq, hw), BF16),
        vm((layers, 4 * rank, hw), BF16),
        vm((layers, 1, hw), F32),
        vm((cols, pad, 128), F32),
        vm((pad, 128), F32),
        vm((4 * rank, rows), BF16),
        vm((cols, 4 * rank, rows), BF16),
        vm((4 * rank, rows), BF16),
        vm((chips, seqs, seq, hw), BF16),
        vm((chips, seqs, seq, hw), BF16),
        vm((seqs, seq, hw), F32),
        vm((seqs, seq, hw), F32),
        vm((chips, seqs, seq, hw), BF16),
        vm((chips, seqs, seq, hw), BF16),
        vm((seqs, seq, hw), F32),
        vm((pads, 128), F32),
        vm((cols, pads, 128), F32),
        vm((pads, 128), F32),
        vm((layers, planes, 4 * rank, hw), BF16),
        vm((layers, 4 * rank, hw), F32),
    ]
    semaphores = [
        dma((cols,)), dma((cols,)), dma((cols,)), dma((cols,)), dma((cols,)), dma((cols,)),
        dma((layers,)), dma((layers,)), dma((layers,)), dma((layers,)), dma((1,)), dma((2,)), dma,
        dma((cols,)), dma((cols,)),
        dma((layers, 4)), dma((layers, planes)), dma((layers, planes)),
        dma((cols,)), dma((cols,)), dma((chips,)), dma((chips,)), dma((chips,)), dma((chips,)),
        dma((cols,)), dma((cols,)), dma((PAIR,)), dma((cols,)),
        dma((layers, planes)), dma((layers, planes)), dma((layers, PAIR)), dma((cols,)),
    ]
    total_scale = (micro * batch * seq) ** (-0.5)
    any_space = pl.BlockSpec(memory_space=pl.ANY)
    input_grad, grads = pl.pallas_call(
        functools.partial(kernel, n_dp, layers, micro, seq, features, rank, rows_w, total_scale),
        out_shape=(
            jax.ShapeDtypeStruct(hidden.shape, BF16),
            jax.ShapeDtypeStruct((4 * rank, features), F32),
        ),
        in_specs=[any_space] * len(args),
        out_specs=(any_space, any_space),
        scratch_shapes=scratch + semaphores,
        compiler_params=pltpu.CompilerParams(
            collective_id=0, has_side_effects=True, vmem_limit_bytes=60 * 1024 * 1024
        ),
        name="section_backward",
    )(*args)
    return (
        input_grad,
        grads[None, :rank],
        grads[None, 2 * rank : 3 * rank],
        grads[None, rank : 2 * rank],
        grads[None, 3 * rank :],
    )


def solution(mesh):
    rows = P("section", None, "dp", None, None)
    cut = P("section", "dp", None)
    small = P("section", None, None)
    return jax.shard_map(
        functools.partial(on_device, mesh.shape["dp"], mesh.shape["section"]),
        mesh=mesh,
        in_specs=(rows,) * 4 + (P(None, "dp", None, None), P("section", None)) + (cut,) * 3 + (small,) * 4,
        out_specs=(rows,) + (small,) * 4,
        check_vma=False,
    )
```

```python
import functools

import jax
import jax.numpy as jnp
from jax import lax
from jax.experimental import pallas as pl
from jax.experimental.pallas import tpu as pltpu
from jax.sharding import PartitionSpec as P

HEAD_DIM = 128
adapter_scale = 2.0
norm_eps = 1e-05
NN = (((1,), (0,)), ((), ()))
NT = (((1,), (1,)), ((), ()))
TN = (((0,), (0,)), ((), ()))
F32 = jnp.float32
BF16 = jnp.bfloat16
MESH = pl.DeviceIdType.MESH
PAIR = 2


def dot(a, b, dims):
    return lax.dot_general(a, b, dims, preferred_element_type=F32)


def drain(ref, sem):
    pltpu.make_async_copy(ref, ref, sem).wait()


def remote(src, dst, send, recv, device):
    return pltpu.make_async_remote_copy(
        src_ref=src, dst_ref=dst, send_sem=send, recv_sem=recv, device_id=device, device_id_type=MESH
    )


def flip(value, k, size):
    if size & (size - 1):
        return lax.rem(value + k, size)
    out, bit = 0, 1
    while bit < size:
        out = out + bit * lax.rem(lax.div(value, bit) + (k // bit) % 2, 2)
        bit *= 2
    return out


def kernel(
    n_dp, layers, micro, seq, features, rank, rows_w, total_scale,
    hid, que, key, val, cot, gain, wq, wk, wv, dq, uq, dv, uv,
    out_ig, out_g,
    wbuf, act, hown, og, ab, nrm, ad, gn, st, st_own, lows, lowr, norms, normr, lowt,
    cs, crecv, ctmp, xs, xrecv, sc, rs_own, rsr, crow, gr, gf,
    w_s, w_r, q_s, q_r, h_s, h_r, ad_s, ad_r, gn_s, gn_r, cot_s, cot_r, hown_sem, st_s, st_r,
    z_s, z_r, rel_s, lo_s, lo_r, ln_s, ln_r, d_s, d_r, x_s, x_r, rs_s, rs_r, o_s, o_r, g_s, g_r, f_s, f_r,
):
    sections = layers
    planes = n_dp // PAIR
    cols = PAIR * sections
    chips = cols // 2
    hw = features // cols
    heads = hw // HEAD_DIM
    seqs = PAIR * micro
    block = PAIR * rows_w
    groups = 2 * heads
    spread = chips * HEAD_DIM
    dp, s = lax.axis_index("dp"), lax.axis_index("section")
    a, x = lax.div(dp, PAIR), lax.rem(dp, PAIR)
    f = x * sections + s
    c = lax.rem(f, 2)
    chip = lax.div(f, 2)

    def device(j):
        return (PAIR * a + lax.div(j, sections), lax.rem(j, sections))

    others = [flip(f, k, cols) for k in range(1, cols)]

    def wide(j, ref):
        for u in range(heads):
            at = ((lax.rem(j, 2) * heads + u) * chips + lax.div(j, 2)) * HEAD_DIM
            yield ref.at[..., pl.ds(pl.multiple_of(at, HEAD_DIM), HEAD_DIM)], pl.ds(u * HEAD_DIM, HEAD_DIM)

    barrier = pltpu.get_barrier_semaphore()
    for j in others:
        pl.semaphore_signal(barrier, inc=1, device_id=device(j), device_id_type=MESH)
    for k in range(1, planes):
        pl.semaphore_signal(
            barrier, inc=1, device_id=(PAIR * lax.rem(a + k, planes) + x, s), device_id_type=MESH
        )
    pl.semaphore_wait(barrier, cols - 1 + planes - 1)

    own_hidden = pltpu.make_async_copy(hid.at[0, :, 0], hown, hown_sem)
    own_hidden.start()
    for k in range(sections):
        s2 = s if k == 0 else flip(s, k, sections)
        j = x * sections + s2
        for i, ref in enumerate((dq, dv, uq, uv)):
            for src, at in wide(j, ref.at[0]):
                dst = ad.at[s, pl.ds(i * rank, rank), at]
                if k == 0:
                    pltpu.make_async_copy(src, dst, ad_r.at[s]).start()
                else:
                    remote(src, dst, ad_s.at[k], ad_r.at[s], (dp, s2)).start()
        for src, at in wide(j, gain):
            dst = gn.at[s, :, at]
            if k == 0:
                pltpu.make_async_copy(src, dst, gn_r.at[s]).start()
            else:
                remote(src, dst, gn_s.at[k], gn_r.at[s], (dp, s2)).start()
    mirror = (PAIR * a + 1 - x, s)
    for src, at in wide((1 - x) * sections + s, cot.at[:, 0]):
        remote(src, og.at[x, :, :, at], cot_s.at[0], cot_r.at[0], mirror).start()
    for src, at in wide(f, cot.at[:, 0]):
        pltpu.make_async_copy(src, og.at[x, :, :, at], cot_r.at[1]).start()

    def weights(j):
        for i, ref in enumerate((wq, wk, wv)):
            for u, (src, at) in enumerate(wide(j, ref.at[0])):
                yield src, wbuf.at[s, a, pl.ds(x * rows_w, rows_w), pl.ds(i * hw + u * HEAD_DIM, HEAD_DIM)]

    def saved(j, which=(0, 1, 2)):
        for i in which:
            for src, at in wide(j, (que, key, val)[i].at[0, :, 0]):
                yield src, act.at[s, x, i, :, :, at]

    def inputs(j):
        for src, at in wide(j, hid.at[0, :, 0]):
            yield src, act.at[s, x, 3, :, :, at]

    for group, recv in ((weights, w_r), (saved, q_r), (inputs, h_r)):
        for src, dst in group(f):
            pltpu.make_async_copy(src, dst, recv.at[f]).start()

    def spread_out(group, send, recv):
        for k, j in enumerate(others):
            for src, dst in group(j):
                remote(src, dst, send.at[k], recv.at[f], device(j)).start()

    early = lax.rem(layers - 1 - s, 2) == 0
    spread_out(weights, w_s, w_r)

    @pl.when(early)
    def _():
        spread_out(saved, q_s, q_r)
        spread_out(inputs, h_s, h_r)

    def z_half(l, xx):
        part = wbuf.at[l, a, pl.ds(xx * rows_w, rows_w), :]
        drain(part, w_r.at[xx * sections + l])
        for i, d in enumerate((2, -2, 1, -1)):
            if abs(d) >= planes:
                continue

            @pl.when((a + d >= 0) & (a + d < planes))
            def _():
                remote(part, part, z_s.at[l, i], z_r.at[l, a], (PAIR * (a + d) + x, s)).start()

    z_half(s, x)

    def z_own(l):
        for xx in range(PAIR):

            @pl.when((l != s) | (xx != x))
            def _():
                z_half(l, xx)

    eye = lax.broadcasted_iota(jnp.int32, (seq, 128), 0) == lax.broadcasted_iota(jnp.int32, (seq, 128), 1)

    def to_row(column):
        return jnp.sum(jnp.where(eye, column, 0.0), axis=0, keepdims=True)

    def to_column(row):
        return jnp.sum(jnp.where(eye, row, 0.0), axis=1, keepdims=True)

    own_hidden.wait()

    def inverse_of(m, carry):
        floated = hown[m].astype(F32)
        inverse = lax.rsqrt(jnp.mean(floated * floated, axis=-1, keepdims=True) + norm_eps)
        st_own[pl.ds(m, 1), :] = to_row(inverse)
        return carry

    lax.fori_loop(0, micro, inverse_of, 0)
    st[f] = st_own[...]
    for k, j in enumerate(others):
        remote(st_own, st.at[f], st_s.at[k], st_r.at[f], device(j)).start()

    def passed_on(l, b, todo):
        for direction in (1, -1):

            @pl.when(((a - b) * direction >= 2) & (a + direction >= 0) & (a + direction < planes))
            def _():
                todo(
                    remote(
                        wbuf.at[l, b], wbuf.at[l, b], rel_s.at[l, b], z_r.at[l, b],
                        (PAIR * (a + direction) + x, s),
                    )
                )

    def take(l, b):
        drain(wbuf.at[l, b], z_r.at[l, b])
        passed_on(l, b, lambda copy: copy.start())

    scale = HEAD_DIM ** (-0.5)
    causal = lax.broadcasted_iota(jnp.int32, (seq, seq), 1) <= lax.broadcasted_iota(jnp.int32, (seq, seq), 0)
    z_own(layers - 1)

    def finish_grads(l):
        for k in range(1, planes):
            b = lax.rem(a + k, planes)
            drain(gr.at[l, b], g_r.at[l, b])
        total = gr[l, 0].astype(F32)
        for b in range(1, planes):
            total = total + gr[l, b].astype(F32)
        gf[l] = total * total_scale
        for xx in range(PAIR):
            mine = (x == xx) & (s == l)
            for dst, at in wide(f, out_g):

                @pl.when(mine)
                def _():
                    pltpu.make_async_copy(gf.at[l, :, at], dst, f_s.at[l, xx]).start()

                @pl.when(jnp.logical_not(mine))
                def _():
                    remote(gf.at[l, :, at], dst, f_s.at[l, xx], f_r.at[f], (PAIR * a + xx, l)).start()

    def layer(i, carry):
        l = layers - 1 - i
        for xx in range(PAIR):
            drain(act.at[l, xx, pl.ds(0, 3)], q_r.at[xx * sections + l])

        @pl.when(i == 0)
        def _():
            @pl.when(jnp.logical_not(early))
            def _():
                spread_out(lambda j: saved(j, (0, 1)), q_s, q_r)

            drain(og.at[0], cot_r.at[0])
            drain(og.at[0], cot_r.at[1])

        def next_own():
            @pl.when(l > 0)
            def _():
                z_own(l - 1)

        ordered = planes == 4 and groups == 4
        upper = lax.div(a, 2)
        near = a + upper * (3 - 2 * a)
        relays = (a == 1) | (a == 2)

        def nearest(k):
            lower = lax.rem(near + k, 2) if k < 2 else k
            return lower + upper * (3 - 2 * lower)

        if ordered:

            @pl.when(relays & (i > 0))
            def _():
                take(l, nearest(3))

            pl.when(i > 0)(next_own)

        def attention(n, carry):
            xx, m = lax.div(n, micro), lax.rem(n, micro)
            for h in range(heads):
                at = pl.ds(h * HEAD_DIM, HEAD_DIM)
                q, k, v = (act[l, xx, t, m, :, at] for t in range(3))
                g = og[xx, m, :, at]
                scores = jnp.where(causal, dot(q, k, NT) * scale, -1e30)
                grown = jnp.exp(scores - jnp.max(scores, axis=-1, keepdims=True))
                attend = grown / jnp.sum(grown, axis=-1, keepdims=True)
                attend_grad = dot(g, v, NT)
                value_grad = dot(attend.astype(BF16), g, TN)
                row_total = jnp.sum(attend * attend_grad, axis=-1, keepdims=True)
                score_grad = (attend * (attend_grad - row_total) * scale).astype(BF16)
                ab[n, :, at] = dot(score_grad, k, NN).astype(BF16)
                ab[n, :, pl.ds(hw + h * HEAD_DIM, HEAD_DIM)] = dot(score_grad, q, TN).astype(BF16)
                ab[n, :, pl.ds(2 * hw + h * HEAD_DIM, HEAD_DIM)] = value_grad.astype(BF16)
            return carry

        lax.fori_loop(0, seqs, attention, 0)

        def flat(value):
            return value.reshape(-1, value.shape[-1])

        if ordered:

            @pl.when(relays & (i == 0))
            def _():
                take(l, nearest(3))

            pl.when(i == 0)(next_own)

        drain(ad.at[l], ad_r.at[l])
        lows[:rank] = (adapter_scale * dot(ad[l, 2 * rank : 3 * rank], flat(ab[:, :, :hw]), NT)).astype(BF16)
        lows[rank:] = (adapter_scale * dot(ad[l, 3 * rank :], flat(ab[:, :, 2 * hw :]), NT)).astype(BF16)
        for k, j in enumerate(others):
            remote(lows, lowr.at[f], lo_s.at[k], lo_r.at[f], device(j)).start()
        down = ad[l, : 2 * rank]

        def normalise_all():
            for xx in range(PAIR):
                j = xx * sections + l
                drain(act.at[l, xx, 3], h_r.at[j])

                @pl.when(j != f)
                def _():
                    drain(st.at[j], st_r.at[j])

            drain(gn.at[l], gn_r.at[l])

            def normalise(n, carry):
                xx, m = lax.div(n, micro), lax.rem(n, micro)
                inverse = to_column(st[xx * sections + l, pl.ds(m, 1), :])
                nrm[n] = (act[l, xx, 3, m].astype(F32) * inverse * gn[l]).astype(BF16)
                return carry

            lax.fori_loop(0, seqs, normalise, 0)
            norms[...] = dot(down, flat(nrm[...]), NT).astype(BF16)
            for k, j in enumerate(others):
                remote(norms, normr.at[f], ln_s.at[k], ln_r.at[f], device(j)).start()

        partner = device(flip(f, 1, cols))

        def group(t):
            if spread == block:
                w = wbuf.at[l, t]
            else:
                w = wbuf.at[l, pl.ds(t * (spread // block), spread // block)]

            def half(xx):
                tokens = flat(ab[pl.ds(xx * micro, micro)])
                return dot(tokens, flat(w[...]), NT).reshape(micro, seq, spread)

            cs[t] = half(1 - c).astype(BF16)
            to_partner = remote(cs.at[t], crecv.at[t], d_s.at[t], d_r.at[t], partner)
            to_partner.start()
            ctmp[...] = half(c)
            to_partner.wait_recv()
            total = ctmp[...] + crecv[t].astype(F32)
            core, u = lax.div(t, heads), lax.rem(t, heads)
            for i in range(chips):
                piece = total[:, :, i * HEAD_DIM : (i + 1) * HEAD_DIM].astype(BF16)
                target = 2 * i + core

                @pl.when(target == f)
                def _():
                    xrecv[u, chip, c] = piece

                @pl.when(target != f)
                def _():
                    xs[t, i] = piece
                    remote(
                        xs.at[t, i], xrecv.at[u, chip, c], x_s.at[t, i], x_r.at[u, chip, c], device(target)
                    ).start()

        def summed(own, received, sems):
            for j in others:
                drain(received.at[j], sems.at[j])
            total = own[...].astype(F32)
            for j in others:
                total = total + received[j].astype(F32)
            return total.astype(BF16)

        def gradients():
            lowt[: 2 * rank] = summed(lows, lowr, lo_r)
            lowt[2 * rank :] = summed(norms, normr, ln_r)
            gr[l, a, : 2 * rank] = dot(lowt[: 2 * rank], flat(nrm[...]), NN).astype(BF16)
            gr[l, a, 2 * rank : 3 * rank] = (
                adapter_scale * dot(lowt[2 * rank : 3 * rank], flat(ab[:, :, :hw]), NN)
            ).astype(BF16)
            gr[l, a, 3 * rank :] = (
                adapter_scale * dot(lowt[3 * rank :], flat(ab[:, :, 2 * hw :]), NN)
            ).astype(BF16)
            for k in range(1, planes):
                there = (PAIR * lax.rem(a + k, planes) + x, s)
                remote(gr.at[l, a], gr.at[l, a], g_s.at[l, k], g_r.at[l, a], there).start()
            sc[...] = dot(lowt[: 2 * rank], down, TN).reshape(seqs, seq, hw)

        if ordered:
            pl.when(i > 0)(normalise_all)
            for k in range(4):
                t = nearest(k)
                if k == 1 or k == 2:
                    take(l, t)
                if k == 3:
                    pl.when(i == 0)(normalise_all)
                    gradients()

                    @pl.when(jnp.logical_not(relays))
                    def _():
                        take(l, t)

                group(t)
        else:
            for d in range(1, planes):
                for b in (a - d, a + d):

                    @pl.when((b >= 0) & (b < planes))
                    def _():
                        take(l, b)

            next_own()
            normalise_all()
            gradients()
            for t in range(groups):
                group(jnp.int32(t))
        pl.when(l == 0)(functools.partial(finish_grads, 0))

        for u in range(heads):
            for j in range(chips):
                for cc in range(2):

                    @pl.when((j != chip) | (cc != c))
                    def _():
                        drain(xrecv.at[u, j, cc], x_r.at[u, j, cc])

        def gather_up(n, carry):
            xx, m = lax.div(n, micro), lax.rem(n, micro)
            sums = []
            for u in range(heads):
                value = sc[n, :, u * HEAD_DIM : (u + 1) * HEAD_DIM]
                for j in range(chips):
                    value = value + xrecv[u, j, xx, m].astype(F32)
                value = gn[l, :, u * HEAD_DIM : (u + 1) * HEAD_DIM] * value
                sc[n, :, u * HEAD_DIM : (u + 1) * HEAD_DIM] = value
                sums.append(act[l, xx, 3, m, :, u * HEAD_DIM : (u + 1) * HEAD_DIM].astype(F32) * value)
            rs_own[pl.ds(n, 1), :] = to_row(jnp.sum(sum(sums), axis=-1, keepdims=True))
            return carry

        lax.fori_loop(0, seqs, gather_up, 0)
        for k, j in enumerate(others):
            remote(rs_own, rsr.at[f], rs_s.at[k], rs_r.at[f], device(j)).start()
        for j in others:
            drain(rsr.at[j], rs_r.at[j])
        correction = rs_own[...]
        for j in others:
            correction = correction + rsr[j]
        crow[...] = correction * (1.0 / features)

        @pl.when(i > 0)
        def _():
            for xx in range(PAIR):
                drain(og.at[xx], o_s.at[xx])

        def settle(n, carry):
            xx, m = lax.div(n, micro), lax.rem(n, micro)
            inverse = to_column(st[xx * sections + l, pl.ds(m, 1), :])
            corrected = to_column(crow[pl.ds(n, 1), :])
            hidden = act[l, xx, 3, m].astype(F32)
            og[xx, m] = (
                og[xx, m].astype(F32) + inverse * sc[n] - hidden * (inverse * inverse * inverse * corrected)
            ).astype(BF16)
            return carry

        lax.fori_loop(0, seqs, settle, 0)

        @pl.when(i == 0)
        def _():
            @pl.when(jnp.logical_not(early))
            def _():
                spread_out(lambda j: saved(j, (2,)), q_s, q_r)
                spread_out(inputs, h_s, h_r)

        for xx in range(PAIR):
            mine = (x == xx) & (s == l)
            for dst, at in wide(f, out_ig.at[0, :, 0]):
                src = og.at[xx, :, :, at]

                @pl.when(mine)
                def _():
                    pltpu.make_async_copy(src, dst, o_s.at[xx]).start()

                @pl.when(jnp.logical_not(mine))
                def _():
                    remote(src, dst, o_s.at[xx], o_r.at[f], (PAIR * a + xx, l)).start()

        @pl.when(i > 0)
        def _():
            finish_grads(l + 1)

        for k in range(cols - 1):
            drain(lows, lo_s.at[k])
            drain(norms, ln_s.at[k])
            drain(rs_own, rs_s.at[k])
        for t in range(groups):
            drain(cs.at[t], d_s.at[t])
            for j in range(chips):

                @pl.when(2 * j + t // heads != f)
                def _():
                    drain(xs.at[t, j], x_s.at[t, j])

        return carry

    lax.fori_loop(0, layers, layer, 0)

    for xx in range(PAIR):
        drain(og.at[xx], o_s.at[xx])
    for j in others:
        drain(og.at[0], o_r.at[j])
        drain(gf.at[0], f_r.at[j])
    for k in range(1, sections):
        drain(ad.at[0], ad_s.at[k])
        drain(gn.at[0], gn_s.at[k])
    drain(og.at[0], cot_s.at[0])
    for k in range(cols - 1):
        drain(wbuf.at[0, 0, pl.ds(0, rows_w), :], w_s.at[k])
        drain(act.at[0, 0, pl.ds(0, 3)], q_s.at[k])
        drain(act.at[0, 0, 3], h_s.at[k])
        drain(st_own, st_s.at[k])

    def sent(l, carry):
        for i, d in enumerate((2, -2, 1, -1)):
            if abs(d) >= planes:
                continue

            @pl.when((a + d >= 0) & (a + d < planes))
            def _():
                drain(wbuf.at[l, a], z_s.at[l, i])

        for d in range(2, planes):
            for b in (a - d, a + d):

                @pl.when((b >= 0) & (b < planes))
                def _():
                    passed_on(l, b, lambda copy: copy.wait_send())

        for k in range(1, planes):
            drain(gr.at[l, a], g_s.at[l, k])
        for xx in range(PAIR):
            drain(gf.at[l], f_s.at[l, xx])
        return carry

    lax.fori_loop(0, layers, sent, 0)


def on_device(n_dp, layers, *args):
    hidden, cot, w, down = args[0], args[4], args[6], args[9]
    micro, seq, features = cot.shape[0], cot.shape[2], cot.shape[3]
    batch = cot.shape[1] * n_dp
    rank, rows_w = down.shape[1], w.shape[1]
    planes, cols = n_dp // PAIR, PAIR * layers
    chips, hw, seqs = cols // 2, features // cols, PAIR * micro
    heads = hw // HEAD_DIM
    groups, spread = 2 * heads, chips * HEAD_DIM
    rows = seqs * seq
    pad = -(-micro // 8) * 8
    pads = -(-seqs // 8) * 8
    dma = pltpu.SemaphoreType.DMA
    vm = pltpu.VMEM
    scratch = [
        vm((layers, planes, PAIR * rows_w, 3 * hw), BF16),
        vm((layers, PAIR, 4, micro, seq, hw), BF16),
        vm((micro, seq, features), BF16),
        vm((PAIR, micro, seq, hw), BF16),
        vm((seqs, seq, 3 * hw), BF16),
        vm((seqs, seq, hw), BF16),
        vm((layers, 4 * rank, hw), BF16),
        vm((layers, 1, hw), F32),
        vm((cols, pad, 128), F32),
        vm((pad, 128), F32),
        vm((2 * rank, rows), BF16),
        vm((cols, 2 * rank, rows), BF16),
        vm((2 * rank, rows), BF16),
        vm((cols, 2 * rank, rows), BF16),
        vm((4 * rank, rows), BF16),
        vm((groups, micro, seq, spread), BF16),
        vm((groups, micro, seq, spread), BF16),
        vm((micro, seq, spread), F32),
        vm((groups, chips, micro, seq, HEAD_DIM), BF16),
        vm((heads, chips, 2, micro, seq, HEAD_DIM), BF16),
        vm((seqs, seq, hw), F32),
        vm((pads, 128), F32),
        vm((cols, pads, 128), F32),
        vm((pads, 128), F32),
        vm((layers, planes, 4 * rank, hw), BF16),
        vm((layers, 4 * rank, hw), F32),
    ]
    semaphores = [
        dma((cols,)), dma((cols,)), dma((cols,)), dma((cols,)), dma((cols,)), dma((cols,)),
        dma((layers,)), dma((layers,)), dma((layers,)), dma((layers,)), dma((1,)), dma((2,)), dma,
        dma((cols,)), dma((cols,)),
        dma((layers, 4)), dma((layers, planes)), dma((layers, planes)),
        dma((cols,)), dma((cols,)), dma((cols,)), dma((cols,)), dma((groups,)), dma((groups,)),
        dma((groups, chips)), dma((heads, chips, 2)),
        dma((cols,)), dma((cols,)), dma((PAIR,)), dma((cols,)),
        dma((layers, planes)), dma((layers, planes)), dma((layers, PAIR)), dma((cols,)),
    ]
    total_scale = (micro * batch * seq) ** (-0.5)
    any_space = pl.BlockSpec(memory_space=pl.ANY)
    input_grad, grads = pl.pallas_call(
        functools.partial(kernel, n_dp, layers, micro, seq, features, rank, rows_w, total_scale),
        out_shape=(
            jax.ShapeDtypeStruct(hidden.shape, BF16),
            jax.ShapeDtypeStruct((4 * rank, features), F32),
        ),
        in_specs=[any_space] * len(args),
        out_specs=(any_space, any_space),
        scratch_shapes=scratch + semaphores,
        compiler_params=pltpu.CompilerParams(
            collective_id=0, has_side_effects=True, vmem_limit_bytes=60 * 1024 * 1024
        ),
        name="section_backward",
    )(*args)
    return (
        input_grad,
        grads[None, :rank],
        grads[None, 2 * rank : 3 * rank],
        grads[None, rank : 2 * rank],
        grads[None, 3 * rank :],
    )


def solution(mesh):
    rows = P("section", None, "dp", None, None)
    cut = P("section", "dp", None)
    small = P("section", None, None)
    return jax.shard_map(
        functools.partial(on_device, mesh.shape["dp"], mesh.shape["section"]),
        mesh=mesh,
        in_specs=(rows,) * 4 + (P(None, "dp", None, None), P("section", None)) + (cut,) * 3 + (small,) * 4,
        out_specs=(rows,) + (small,) * 4,
        check_vma=False,
    )
```

```python
import functools

import jax
import jax.numpy as jnp
from jax import lax
from jax.experimental import pallas as pl
from jax.experimental.pallas import tpu as pltpu
from jax.sharding import PartitionSpec as P

HEAD_DIM = 128
adapter_scale = 2.0
norm_eps = 1e-05
NN = (((1,), (0,)), ((), ()))
NT = (((1,), (1,)), ((), ()))
TN = (((0,), (0,)), ((), ()))
F32 = jnp.float32
BF16 = jnp.bfloat16
MESH = pl.DeviceIdType.MESH
PAIR = 2


def dot(a, b, dims):
    return lax.dot_general(a, b, dims, preferred_element_type=F32)


def drain(ref, sem):
    pltpu.make_async_copy(ref, ref, sem).wait()


def remote(src, dst, send, recv, device):
    return pltpu.make_async_remote_copy(
        src_ref=src, dst_ref=dst, send_sem=send, recv_sem=recv, device_id=device, device_id_type=MESH
    )


def flip(value, k, size):
    if size & (size - 1):
        return lax.rem(value + k, size)
    out, bit = 0, 1
    while bit < size:
        out = out + bit * lax.rem(lax.div(value, bit) + (k // bit) % 2, 2)
        bit *= 2
    return out


def kernel(
    n_dp, layers, micro, seq, features, rank, rows_w, total_scale,
    hid, que, key, val, cot, gain, wq, wk, wv, dq, uq, dv, uv,
    out_ig, out_g,
    wbuf, act, hown, og, ab, nrm, ad, gn, st, st_own, both, pair_r, pair_t, chip_r, lowt,
    cs, crecv, ctmp, xs, xrecv, sc, rs_own, rsr, crow, gr, gf,
    w_s, w_r, q_s, q_r, h_s, h_r, ad_s, ad_r, gn_s, gn_r, cot_s, cot_r, hown_sem, st_s, st_r,
    z_s, z_r, rel_s, lp_s, lp_r, lx_s, lx_r, lt_s, lt_r, d_s, d_r, x_s, x_r, rs_s, rs_r, o_s, o_r, g_s, g_r, f_s, f_r,
):
    sections = layers
    planes = n_dp // PAIR
    cols = PAIR * sections
    chips = cols // 2
    hw = features // cols
    heads = hw // HEAD_DIM
    seqs = PAIR * micro
    block = PAIR * rows_w
    groups = 2 * heads
    spread = chips * HEAD_DIM
    dp, s = lax.axis_index("dp"), lax.axis_index("section")
    a, x = lax.div(dp, PAIR), lax.rem(dp, PAIR)
    f = x * sections + s
    c = lax.rem(f, 2)
    chip = lax.div(f, 2)

    def device(j):
        return (PAIR * a + lax.div(j, sections), lax.rem(j, sections))

    others = [flip(f, k, cols) for k in range(1, cols)]

    def wide(j, ref):
        for u in range(heads):
            at = ((lax.rem(j, 2) * heads + u) * chips + lax.div(j, 2)) * HEAD_DIM
            yield ref.at[..., pl.ds(pl.multiple_of(at, HEAD_DIM), HEAD_DIM)], pl.ds(u * HEAD_DIM, HEAD_DIM)

    barrier = pltpu.get_barrier_semaphore()
    for j in others:
        pl.semaphore_signal(barrier, inc=1, device_id=device(j), device_id_type=MESH)
    for k in range(1, planes):
        pl.semaphore_signal(
            barrier, inc=1, device_id=(PAIR * lax.rem(a + k, planes) + x, s), device_id_type=MESH
        )
    pl.semaphore_wait(barrier, cols - 1 + planes - 1)

    own_hidden = pltpu.make_async_copy(hid.at[0, :, 0], hown, hown_sem)
    own_hidden.start()
    for k in range(sections):
        s2 = s if k == 0 else flip(s, k, sections)
        j = x * sections + s2
        for i, ref in enumerate((dq, dv, uq, uv)):
            for src, at in wide(j, ref.at[0]):
                dst = ad.at[s, pl.ds(i * rank, rank), at]
                if k == 0:
                    pltpu.make_async_copy(src, dst, ad_r.at[s]).start()
                else:
                    remote(src, dst, ad_s.at[k], ad_r.at[s], (dp, s2)).start()
        for src, at in wide(j, gain):
            dst = gn.at[s, :, at]
            if k == 0:
                pltpu.make_async_copy(src, dst, gn_r.at[s]).start()
            else:
                remote(src, dst, gn_s.at[k], gn_r.at[s], (dp, s2)).start()
    mirror = (PAIR * a + 1 - x, s)
    for src, at in wide((1 - x) * sections + s, cot.at[:, 0]):
        remote(src, og.at[x, :, :, at], cot_s.at[0], cot_r.at[0], mirror).start()
    for src, at in wide(f, cot.at[:, 0]):
        pltpu.make_async_copy(src, og.at[x, :, :, at], cot_r.at[1]).start()

    def weights(j):
        for i, ref in enumerate((wq, wk, wv)):
            for u, (src, at) in enumerate(wide(j, ref.at[0])):
                yield src, wbuf.at[s, a, pl.ds(x * rows_w, rows_w), pl.ds(i * hw + u * HEAD_DIM, HEAD_DIM)]

    def saved(j, which=(0, 1, 2)):
        for i in which:
            for src, at in wide(j, (que, key, val)[i].at[0, :, 0]):
                yield src, act.at[s, x, i, :, :, at]

    def inputs(j):
        for src, at in wide(j, hid.at[0, :, 0]):
            yield src, act.at[s, x, 3, :, :, at]

    for group, recv in ((weights, w_r), (saved, q_r), (inputs, h_r)):
        for src, dst in group(f):
            pltpu.make_async_copy(src, dst, recv.at[f]).start()

    def spread_out(group, send, recv):
        for k, j in enumerate(others):
            for src, dst in group(j):
                remote(src, dst, send.at[k], recv.at[f], device(j)).start()

    early = lax.rem(layers - 1 - s, 2) == 0

    @pl.when(early)
    def _():
        spread_out(weights, w_s, w_r)
        spread_out(saved, q_s, q_r)
        spread_out(inputs, h_s, h_r)

    def z_half(l, xx):
        part = wbuf.at[l, a, pl.ds(xx * rows_w, rows_w), :]
        drain(part, w_r.at[xx * sections + l])
        for i, d in enumerate((2, -2, 1, -1)):
            if abs(d) >= planes:
                continue

            @pl.when((a + d >= 0) & (a + d < planes))
            def _():
                remote(part, part, z_s.at[l, i], z_r.at[l, a], (PAIR * (a + d) + x, s)).start()

    z_half(s, x)

    def z_own(l):
        for xx in range(PAIR):

            @pl.when((l != s) | (xx != x))
            def _():
                z_half(l, xx)

    eye = lax.broadcasted_iota(jnp.int32, (seq, 128), 0) == lax.broadcasted_iota(jnp.int32, (seq, 128), 1)

    def to_row(column):
        return jnp.sum(jnp.where(eye, column, 0.0), axis=0, keepdims=True)

    def to_column(row):
        return jnp.sum(jnp.where(eye, row, 0.0), axis=1, keepdims=True)

    own_hidden.wait()

    def inverse_of(m, carry):
        floated = hown[m].astype(F32)
        inverse = lax.rsqrt(jnp.mean(floated * floated, axis=-1, keepdims=True) + norm_eps)
        st_own[pl.ds(m, 1), :] = to_row(inverse)
        return carry

    lax.fori_loop(0, micro, inverse_of, 0)
    st[f] = st_own[...]
    for k, j in enumerate(others):
        remote(st_own, st.at[f], st_s.at[k], st_r.at[f], device(j)).start()

    def passed_on(l, b, todo):
        for direction in (1, -1):

            @pl.when(((a - b) * direction >= 2) & (a + direction >= 0) & (a + direction < planes))
            def _():
                todo(
                    remote(
                        wbuf.at[l, b], wbuf.at[l, b], rel_s.at[l, b], z_r.at[l, b],
                        (PAIR * (a + direction) + x, s),
                    )
                )

    def take(l, b):
        drain(wbuf.at[l, b], z_r.at[l, b])
        passed_on(l, b, lambda copy: copy.start())

    scale = HEAD_DIM ** (-0.5)
    causal = lax.broadcasted_iota(jnp.int32, (seq, seq), 1) <= lax.broadcasted_iota(jnp.int32, (seq, seq), 0)
    z_own(layers - 1)

    def finish_grads(l):
        for k in range(1, planes):
            b = lax.rem(a + k, planes)
            drain(gr.at[l, b], g_r.at[l, b])
        total = gr[l, 0].astype(F32)
        for b in range(1, planes):
            total = total + gr[l, b].astype(F32)
        gf[l] = total * total_scale
        for xx in range(PAIR):
            mine = (x == xx) & (s == l)
            for dst, at in wide(f, out_g):

                @pl.when(mine)
                def _():
                    pltpu.make_async_copy(gf.at[l, :, at], dst, f_s.at[l, xx]).start()

                @pl.when(jnp.logical_not(mine))
                def _():
                    remote(gf.at[l, :, at], dst, f_s.at[l, xx], f_r.at[f], (PAIR * a + xx, l)).start()

    def layer(i, carry):
        l = layers - 1 - i
        ordered = planes == 4 and groups == 4
        upper = lax.div(a, 2)
        near = a + upper * (3 - 2 * a)
        relays = (a == 1) | (a == 2)

        def nearest(k):
            lower = lax.rem(near + k, 2) if k < 2 else k
            return lower + upper * (3 - 2 * lower)

        def pass_layer(m):
            @pl.when(relays)
            def _():
                take(m, nearest(3))

        def next_own(m):
            @pl.when(m > 0)
            def _():
                z_own(m - 1)

        if ordered:

            @pl.when((i == 1) | (i > 2))
            def _():
                pass_layer(l)
                next_own(l)

        for xx in range(PAIR):
            drain(act.at[l, xx, pl.ds(0, 3)], q_r.at[xx * sections + l])

        @pl.when(i == 0)
        def _():
            drain(og.at[0], cot_r.at[0])
            drain(og.at[0], cot_r.at[1])

        def attention(n, carry):
            xx, m = lax.div(n, micro), lax.rem(n, micro)
            for h in range(heads):
                at = pl.ds(h * HEAD_DIM, HEAD_DIM)
                q, k, v = (act[l, xx, t, m, :, at] for t in range(3))
                g = og[xx, m, :, at]
                scores = jnp.where(causal, dot(q, k, NT) * scale, -1e30)
                grown = jnp.exp(scores - jnp.max(scores, axis=-1, keepdims=True))
                attend = grown / jnp.sum(grown, axis=-1, keepdims=True)
                attend_grad = dot(g, v, NT)
                value_grad = dot(attend.astype(BF16), g, TN)
                row_total = jnp.sum(attend * attend_grad, axis=-1, keepdims=True)
                score_grad = (attend * (attend_grad - row_total) * scale).astype(BF16)
                ab[n, :, at] = dot(score_grad, k, NN).astype(BF16)
                ab[n, :, pl.ds(hw + h * HEAD_DIM, HEAD_DIM)] = dot(score_grad, q, TN).astype(BF16)
                ab[n, :, pl.ds(2 * hw + h * HEAD_DIM, HEAD_DIM)] = value_grad.astype(BF16)
            return carry

        lax.fori_loop(0, seqs, attention, 0)

        def flat(value):
            return value.reshape(-1, value.shape[-1])

        if ordered:

            @pl.when(i == 0)
            def _():
                pass_layer(l)

        drain(ad.at[l], ad_r.at[l])
        both[0, :rank] = (adapter_scale * dot(ad[l, 2 * rank : 3 * rank], flat(ab[:, :, :hw]), NT)).astype(BF16)
        both[0, rank:] = (adapter_scale * dot(ad[l, 3 * rank :], flat(ab[:, :, 2 * hw :]), NT)).astype(BF16)
        partner = device(flip(f, 1, cols))

        @pl.when(c == 1)
        def _():
            remote(both.at[0], pair_r, lp_s.at[0], lp_r.at[0], partner).start()

        down = ad[l, : 2 * rank]

        def normalise_all():
            for xx in range(PAIR):
                j = xx * sections + l
                drain(act.at[l, xx, 3], h_r.at[j])

                @pl.when(j != f)
                def _():
                    drain(st.at[j], st_r.at[j])

            drain(gn.at[l], gn_r.at[l])

            def normalise(n, carry):
                xx, m = lax.div(n, micro), lax.rem(n, micro)
                inverse = to_column(st[xx * sections + l, pl.ds(m, 1), :])
                nrm[n] = (act[l, xx, 3, m].astype(F32) * inverse * gn[l]).astype(BF16)
                return carry

            lax.fori_loop(0, seqs, normalise, 0)
            both[1] = dot(down, flat(nrm[...]), NT).astype(BF16)

            @pl.when(c == 0)
            def _():
                remote(both.at[1], pair_r, lp_s.at[0], lp_r.at[0], partner).start()

        def over_pair():
            drain(pair_r, lp_r.at[0])
            pair_t[...] = (both[c].astype(F32) + pair_r[...].astype(F32)).astype(BF16)
            for k in range(1, chips):
                target = device(2 * flip(chip, k, chips) + c)
                remote(pair_t, chip_r.at[chip], lx_s.at[k], lx_r.at[chip], target).start()

        def over_chips():
            total = pair_t[...].astype(F32)
            for k in range(1, chips):
                drain(chip_r.at[flip(chip, k, chips)], lx_r.at[flip(chip, k, chips)])
            for k in range(1, chips):
                total = total + chip_r[flip(chip, k, chips)].astype(F32)
            lowt[c] = total.astype(BF16)
            remote(lowt.at[c], lowt.at[c], lt_s.at[0], lt_r.at[0], partner).start()

        def group(t):
            if spread == block:
                w = wbuf.at[l, t]
            else:
                w = wbuf.at[l, pl.ds(t * (spread // block), spread // block)]

            def half(xx):
                tokens = flat(ab[pl.ds(xx * micro, micro)])
                return dot(tokens, flat(w[...]), NT).reshape(micro, seq, spread)

            cs[t] = half(1 - c).astype(BF16)
            to_partner = remote(cs.at[t], crecv.at[t], d_s.at[t], d_r.at[t], partner)
            to_partner.start()
            ctmp[...] = half(c)
            to_partner.wait_recv()
            total = ctmp[...] + crecv[t].astype(F32)
            core, u = lax.div(t, heads), lax.rem(t, heads)
            for i in range(chips):
                piece = total[:, :, i * HEAD_DIM : (i + 1) * HEAD_DIM].astype(BF16)
                target = 2 * i + core

                @pl.when(target == f)
                def _():
                    xrecv[u, chip, c] = piece

                @pl.when(target != f)
                def _():
                    xs[t, i] = piece
                    remote(
                        xs.at[t, i], xrecv.at[u, chip, c], x_s.at[t, i], x_r.at[u, chip, c], device(target)
                    ).start()

        def send_late():
            @pl.when(jnp.logical_not(early))
            def _():
                spread_out(weights, w_s, w_r)
                spread_out(lambda j: saved(j, (0,)), q_s, q_r)

        def gradients():
            drain(lowt.at[1 - c], lt_r.at[0])
            gr[l, a, : 2 * rank] = dot(lowt[0], flat(nrm[...]), NN).astype(BF16)
            gr[l, a, 2 * rank : 3 * rank] = (adapter_scale * dot(lowt[1, :rank], flat(ab[:, :, :hw]), NN)).astype(BF16)
            gr[l, a, 3 * rank :] = (adapter_scale * dot(lowt[1, rank:], flat(ab[:, :, 2 * hw :]), NN)).astype(BF16)
            for k in range(1, planes):
                there = (PAIR * lax.rem(a + k, planes) + x, s)
                remote(gr.at[l, a], gr.at[l, a], g_s.at[l, k], g_r.at[l, a], there).start()
            sc[...] = dot(lowt[0], down, TN).reshape(seqs, seq, hw)

        if ordered:
            pl.when(i > 1)(normalise_all)
            for k in range(4):
                t = nearest(k)
                if k == 1 or k == 2:
                    take(l, t)
                if k == 3:

                    pl.when(i == 0)(functools.partial(next_own, l))
                    pl.when(i < 2)(normalise_all)
                    pl.when((i < 2) & (c == 1))(over_pair)

                    @pl.when(jnp.logical_not(relays))
                    def _():
                        take(l, t)

                group(t)
                if k == 0:
                    pl.when((i > 1) | (c == 0))(over_pair)
                    pl.when(i == 0)(send_late)
        else:
            for d in range(1, planes):
                for b in (a - d, a + d):

                    @pl.when((b >= 0) & (b < planes))
                    def _():
                        take(l, b)

            pl.when(i == 0)(send_late)
            next_own(l)
            normalise_all()
            over_pair()
            for t in range(groups):
                group(jnp.int32(t))
        over_chips()
        gradients()
        if ordered:

            @pl.when((i == 1) & (l > 0))
            def _():
                pass_layer(l - 1)
                next_own(l - 1)

        pl.when(l == 0)(functools.partial(finish_grads, 0))

        for u in range(heads):
            for j in range(chips):
                for cc in range(2):

                    @pl.when((j != chip) | (cc != c))
                    def _():
                        drain(xrecv.at[u, j, cc], x_r.at[u, j, cc])

        def gather_up(n, carry):
            xx, m = lax.div(n, micro), lax.rem(n, micro)
            sums = []
            for u in range(heads):
                value = sc[n, :, u * HEAD_DIM : (u + 1) * HEAD_DIM]
                for j in range(chips):
                    value = value + xrecv[u, j, xx, m].astype(F32)
                value = gn[l, :, u * HEAD_DIM : (u + 1) * HEAD_DIM] * value
                sc[n, :, u * HEAD_DIM : (u + 1) * HEAD_DIM] = value
                sums.append(act[l, xx, 3, m, :, u * HEAD_DIM : (u + 1) * HEAD_DIM].astype(F32) * value)
            rs_own[pl.ds(n, 1), :] = to_row(jnp.sum(sum(sums), axis=-1, keepdims=True))
            return carry

        lax.fori_loop(0, seqs, gather_up, 0)
        for k, j in enumerate(others):
            remote(rs_own, rsr.at[f], rs_s.at[k], rs_r.at[f], device(j)).start()
        for j in others:
            drain(rsr.at[j], rs_r.at[j])
        correction = rs_own[...]
        for j in others:
            correction = correction + rsr[j]
        crow[...] = correction * (1.0 / features)

        @pl.when(i > 0)
        def _():
            for xx in range(PAIR):
                drain(og.at[xx], o_s.at[xx])

        def settle(n, carry):
            xx, m = lax.div(n, micro), lax.rem(n, micro)
            inverse = to_column(st[xx * sections + l, pl.ds(m, 1), :])
            corrected = to_column(crow[pl.ds(n, 1), :])
            hidden = act[l, xx, 3, m].astype(F32)
            og[xx, m] = (
                og[xx, m].astype(F32) + inverse * sc[n] - hidden * (inverse * inverse * inverse * corrected)
            ).astype(BF16)
            return carry

        lax.fori_loop(0, seqs, settle, 0)

        @pl.when(i == 0)
        def _():
            @pl.when(jnp.logical_not(early))
            def _():
                spread_out(lambda j: saved(j, (1, 2)), q_s, q_r)
                spread_out(inputs, h_s, h_r)

        for xx in range(PAIR):
            mine = (x == xx) & (s == l)
            for dst, at in wide(f, out_ig.at[0, :, 0]):
                src = og.at[xx, :, :, at]

                @pl.when(mine)
                def _():
                    pltpu.make_async_copy(src, dst, o_s.at[xx]).start()

                @pl.when(jnp.logical_not(mine))
                def _():
                    remote(src, dst, o_s.at[xx], o_r.at[f], (PAIR * a + xx, l)).start()

        @pl.when(i > 0)
        def _():
            finish_grads(l + 1)

        for k in range(cols - 1):
            drain(rs_own, rs_s.at[k])
        drain(both.at[0], lp_s.at[0])
        drain(lowt.at[0], lt_s.at[0])
        for k in range(1, chips):
            drain(pair_t, lx_s.at[k])
        for t in range(groups):
            drain(cs.at[t], d_s.at[t])
            for j in range(chips):

                @pl.when(2 * j + t // heads != f)
                def _():
                    drain(xs.at[t, j], x_s.at[t, j])

        return carry

    lax.fori_loop(0, layers, layer, 0)

    for xx in range(PAIR):
        drain(og.at[xx], o_s.at[xx])
    for j in others:
        drain(og.at[0], o_r.at[j])
        drain(gf.at[0], f_r.at[j])
    for k in range(1, sections):
        drain(ad.at[0], ad_s.at[k])
        drain(gn.at[0], gn_s.at[k])
    drain(og.at[0], cot_s.at[0])
    for k in range(cols - 1):
        drain(wbuf.at[0, 0, pl.ds(0, rows_w), :], w_s.at[k])
        drain(act.at[0, 0, pl.ds(0, 3)], q_s.at[k])
        drain(act.at[0, 0, 3], h_s.at[k])
        drain(st_own, st_s.at[k])

    def sent(l, carry):
        for i, d in enumerate((2, -2, 1, -1)):
            if abs(d) >= planes:
                continue

            @pl.when((a + d >= 0) & (a + d < planes))
            def _():
                drain(wbuf.at[l, a], z_s.at[l, i])

        for d in range(2, planes):
            for b in (a - d, a + d):

                @pl.when((b >= 0) & (b < planes))
                def _():
                    passed_on(l, b, lambda copy: copy.wait_send())

        for k in range(1, planes):
            drain(gr.at[l, a], g_s.at[l, k])
        for xx in range(PAIR):
            drain(gf.at[l], f_s.at[l, xx])
        return carry

    lax.fori_loop(0, layers, sent, 0)


def on_device(n_dp, layers, *args):
    hidden, cot, w, down = args[0], args[4], args[6], args[9]
    micro, seq, features = cot.shape[0], cot.shape[2], cot.shape[3]
    batch = cot.shape[1] * n_dp
    rank, rows_w = down.shape[1], w.shape[1]
    planes, cols = n_dp // PAIR, PAIR * layers
    chips, hw, seqs = cols // 2, features // cols, PAIR * micro
    heads = hw // HEAD_DIM
    groups, spread = 2 * heads, chips * HEAD_DIM
    rows = seqs * seq
    pad = -(-micro // 8) * 8
    pads = -(-seqs // 8) * 8
    dma = pltpu.SemaphoreType.DMA
    vm = pltpu.VMEM
    scratch = [
        vm((layers, planes, PAIR * rows_w, 3 * hw), BF16),
        vm((layers, PAIR, 4, micro, seq, hw), BF16),
        vm((micro, seq, features), BF16),
        vm((PAIR, micro, seq, hw), BF16),
        vm((seqs, seq, 3 * hw), BF16),
        vm((seqs, seq, hw), BF16),
        vm((layers, 4 * rank, hw), BF16),
        vm((layers, 1, hw), F32),
        vm((cols, pad, 128), F32),
        vm((pad, 128), F32),
        vm((2, 2 * rank, rows), BF16),
        vm((2 * rank, rows), BF16),
        vm((2 * rank, rows), BF16),
        vm((chips, 2 * rank, rows), BF16),
        vm((2, 2 * rank, rows), BF16),
        vm((groups, micro, seq, spread), BF16),
        vm((groups, micro, seq, spread), BF16),
        vm((micro, seq, spread), F32),
        vm((groups, chips, micro, seq, HEAD_DIM), BF16),
        vm((heads, chips, 2, micro, seq, HEAD_DIM), BF16),
        vm((seqs, seq, hw), F32),
        vm((pads, 128), F32),
        vm((cols, pads, 128), F32),
        vm((pads, 128), F32),
        vm((layers, planes, 4 * rank, hw), BF16),
        vm((layers, 4 * rank, hw), F32),
    ]
    semaphores = [
        dma((cols,)), dma((cols,)), dma((cols,)), dma((cols,)), dma((cols,)), dma((cols,)),
        dma((layers,)), dma((layers,)), dma((layers,)), dma((layers,)), dma((1,)), dma((2,)), dma,
        dma((cols,)), dma((cols,)),
        dma((layers, 4)), dma((layers, planes)), dma((layers, planes)),
        dma((1,)), dma((1,)), dma((chips,)), dma((chips,)), dma((1,)), dma((1,)), dma((groups,)), dma((groups,)),
        dma((groups, chips)), dma((heads, chips, 2)),
        dma((cols,)), dma((cols,)), dma((PAIR,)), dma((cols,)),
        dma((layers, planes)), dma((layers, planes)), dma((layers, PAIR)), dma((cols,)),
    ]
    total_scale = (micro * batch * seq) ** (-0.5)
    any_space = pl.BlockSpec(memory_space=pl.ANY)
    input_grad, grads = pl.pallas_call(
        functools.partial(kernel, n_dp, layers, micro, seq, features, rank, rows_w, total_scale),
        out_shape=(
            jax.ShapeDtypeStruct(hidden.shape, BF16),
            jax.ShapeDtypeStruct((4 * rank, features), F32),
        ),
        in_specs=[any_space] * len(args),
        out_specs=(any_space, any_space),
        scratch_shapes=scratch + semaphores,
        compiler_params=pltpu.CompilerParams(
            collective_id=0, has_side_effects=True, vmem_limit_bytes=60 * 1024 * 1024
        ),
        name="section_backward",
    )(*args)
    return (
        input_grad,
        grads[None, :rank],
        grads[None, 2 * rank : 3 * rank],
        grads[None, rank : 2 * rank],
        grads[None, 3 * rank :],
    )


def solution(mesh):
    rows = P("section", None, "dp", None, None)
    cut = P("section", "dp", None)
    small = P("section", None, None)
    return jax.shard_map(
        functools.partial(on_device, mesh.shape["dp"], mesh.shape["section"]),
        mesh=mesh,
        in_specs=(rows,) * 4 + (P(None, "dp", None, None), P("section", None)) + (cut,) * 3 + (small,) * 4,
        out_specs=(rows,) + (small,) * 4,
        check_vma=False,
    )
```

```python
import functools

import jax
import jax.numpy as jnp
from jax import lax
from jax.experimental import pallas as pl
from jax.experimental.pallas import tpu as pltpu
from jax.sharding import PartitionSpec as P

HEAD_DIM = 128
adapter_scale = 2.0
norm_eps = 1e-05
NN = (((1,), (0,)), ((), ()))
NT = (((1,), (1,)), ((), ()))
TN = (((0,), (0,)), ((), ()))
F32 = jnp.float32
BF16 = jnp.bfloat16
MESH = pl.DeviceIdType.MESH
PAIR = 2


def dot(a, b, dims):
    return lax.dot_general(a, b, dims, preferred_element_type=F32)


def drain(ref, sem):
    pltpu.make_async_copy(ref, ref, sem).wait()


def remote(src, dst, send, recv, device):
    return pltpu.make_async_remote_copy(
        src_ref=src, dst_ref=dst, send_sem=send, recv_sem=recv, device_id=device, device_id_type=MESH
    )


def flip(value, k, size):
    if size & (size - 1):
        return lax.rem(value + k, size)
    out, bit = 0, 1
    while bit < size:
        out = out + bit * lax.rem(lax.div(value, bit) + (k // bit) % 2, 2)
        bit *= 2
    return out


def kernel(
    n_dp, layers, micro, seq, features, rank, rows_w, total_scale,
    hid, que, key, val, cot, gain, wq, wk, wv, dq, uq, dv, uv,
    out_ig, out_g,
    wbuf, act, hown, og, ab, nrm, ad, gn, st, st_own, both, pair_r, pair_t, chip_r, lowt,
    cs, crecv, ctmp, xs, xrecv, sc, rs_own, rsr, crow, gr, gf,
    w_s, w_r, q_s, q_r, h_s, h_r, ad_s, ad_r, gn_s, gn_r, cot_s, cot_r, hown_sem, st_s, st_r,
    z_s, z_r, rel_s, lp_s, lp_r, lx_s, lx_r, lt_s, lt_r, d_s, d_r, x_s, x_r, rs_s, rs_r, o_s, o_r, g_s, g_r, f_s, f_r,
):
    sections = layers
    planes = n_dp // PAIR
    cols = PAIR * sections
    chips = cols // 2
    hw = features // cols
    heads = hw // HEAD_DIM
    seqs = PAIR * micro
    block = PAIR * rows_w
    groups = 2 * heads
    spread = chips * HEAD_DIM
    dp, s = lax.axis_index("dp"), lax.axis_index("section")
    a, x = lax.div(dp, PAIR), lax.rem(dp, PAIR)
    f = x * sections + s
    c = lax.rem(f, 2)
    chip = lax.div(f, 2)

    def device(j):
        return (PAIR * a + lax.div(j, sections), lax.rem(j, sections))

    others = [flip(f, k, cols) for k in range(1, cols)]

    def wide(j, ref):
        for u in range(heads):
            at = ((lax.rem(j, 2) * heads + u) * chips + lax.div(j, 2)) * HEAD_DIM
            yield ref.at[..., pl.ds(pl.multiple_of(at, HEAD_DIM), HEAD_DIM)], pl.ds(u * HEAD_DIM, HEAD_DIM)

    barrier = pltpu.get_barrier_semaphore()
    for j in others:
        pl.semaphore_signal(barrier, inc=1, device_id=device(j), device_id_type=MESH)
    for k in range(1, planes):
        pl.semaphore_signal(
            barrier, inc=1, device_id=(PAIR * lax.rem(a + k, planes) + x, s), device_id_type=MESH
        )
    pl.semaphore_wait(barrier, cols - 1 + planes - 1)

    own_hidden = pltpu.make_async_copy(hid.at[0, :, 0], hown, hown_sem)
    own_hidden.start()
    for k in range(sections):
        s2 = s if k == 0 else flip(s, k, sections)
        j = x * sections + s2
        for i, ref in enumerate((dq, dv, uq, uv)):
            for src, at in wide(j, ref.at[0]):
                dst = ad.at[s, pl.ds(i * rank, rank), at]
                if k == 0:
                    pltpu.make_async_copy(src, dst, ad_r.at[s]).start()
                else:
                    remote(src, dst, ad_s.at[k], ad_r.at[s], (dp, s2)).start()
        for src, at in wide(j, gain):
            dst = gn.at[s, :, at]
            if k == 0:
                pltpu.make_async_copy(src, dst, gn_r.at[s]).start()
            else:
                remote(src, dst, gn_s.at[k], gn_r.at[s], (dp, s2)).start()
    mirror = (PAIR * a + 1 - x, s)
    for src, at in wide((1 - x) * sections + s, cot.at[:, 0]):
        remote(src, og.at[x, :, :, at], cot_s.at[0], cot_r.at[0], mirror).start()
    for src, at in wide(f, cot.at[:, 0]):
        pltpu.make_async_copy(src, og.at[x, :, :, at], cot_r.at[1]).start()

    def weights(j):
        for i, ref in enumerate((wq, wk, wv)):
            for u, (src, at) in enumerate(wide(j, ref.at[0])):
                yield src, wbuf.at[s, a, pl.ds(x * rows_w, rows_w), pl.ds(i * hw + u * HEAD_DIM, HEAD_DIM)]

    def saved(j, which=(0, 1, 2)):
        for i in which:
            for src, at in wide(j, (que, key, val)[i].at[0, :, 0]):
                yield src, act.at[s, x, i, :, :, at]

    def inputs(j):
        for src, at in wide(j, hid.at[0, :, 0]):
            yield src, act.at[s, x, 3, :, :, at]

    for group, recv in ((weights, w_r), (saved, q_r), (inputs, h_r)):
        for src, dst in group(f):
            pltpu.make_async_copy(src, dst, recv.at[f]).start()

    def spread_out(group, send, recv):
        for k, j in enumerate(others):
            for src, dst in group(j):
                remote(src, dst, send.at[k], recv.at[f], device(j)).start()

    early = lax.rem(layers - 1 - s, 2) == 0

    @pl.when(early)
    def _():
        spread_out(weights, w_s, w_r)
        spread_out(saved, q_s, q_r)
        spread_out(inputs, h_s, h_r)

    def z_half(l, xx):
        part = wbuf.at[l, a, pl.ds(xx * rows_w, rows_w), :]
        drain(part, w_r.at[xx * sections + l])
        for i, d in enumerate((2, -2, 1, -1)):
            if abs(d) >= planes:
                continue

            @pl.when((a + d >= 0) & (a + d < planes))
            def _():
                remote(part, part, z_s.at[l, i], z_r.at[l, a], (PAIR * (a + d) + x, s)).start()

    z_half(s, x)

    def z_own(l):
        for xx in range(PAIR):

            @pl.when((l != s) | (xx != x))
            def _():
                z_half(l, xx)

    eye = lax.broadcasted_iota(jnp.int32, (seq, 128), 0) == lax.broadcasted_iota(jnp.int32, (seq, 128), 1)

    def to_row(column):
        return jnp.sum(jnp.where(eye, column, 0.0), axis=0, keepdims=True)

    def to_column(row):
        return jnp.sum(jnp.where(eye, row, 0.0), axis=1, keepdims=True)

    own_hidden.wait()

    def inverse_of(m, carry):
        floated = hown[m].astype(F32)
        inverse = lax.rsqrt(jnp.mean(floated * floated, axis=-1, keepdims=True) + norm_eps)
        st_own[pl.ds(m, 1), :] = to_row(inverse)
        return carry

    lax.fori_loop(0, micro, inverse_of, 0)
    st[f] = st_own[...]
    for k, j in enumerate(others):
        remote(st_own, st.at[f], st_s.at[k], st_r.at[f], device(j)).start()

    def passed_on(l, b, todo):
        for direction in (1, -1):

            @pl.when(((a - b) * direction >= 2) & (a + direction >= 0) & (a + direction < planes))
            def _():
                todo(
                    remote(
                        wbuf.at[l, b], wbuf.at[l, b], rel_s.at[l, b], z_r.at[l, b],
                        (PAIR * (a + direction) + x, s),
                    )
                )

    def take(l, b):
        drain(wbuf.at[l, b], z_r.at[l, b])
        passed_on(l, b, lambda copy: copy.start())

    scale = HEAD_DIM ** (-0.5)
    causal = lax.broadcasted_iota(jnp.int32, (seq, seq), 1) <= lax.broadcasted_iota(jnp.int32, (seq, seq), 0)
    z_own(layers - 1)

    def finish_grads(l):
        for k in range(1, planes):
            b = lax.rem(a + k, planes)
            drain(gr.at[l, b], g_r.at[l, b])
        total = gr[l, 0].astype(F32)
        for b in range(1, planes):
            total = total + gr[l, b].astype(F32)
        gf[l] = total * total_scale
        for xx in range(PAIR):
            mine = (x == xx) & (s == l)
            for dst, at in wide(f, out_g):

                @pl.when(mine)
                def _():
                    pltpu.make_async_copy(gf.at[l, :, at], dst, f_s.at[l, xx]).start()

                @pl.when(jnp.logical_not(mine))
                def _():
                    remote(gf.at[l, :, at], dst, f_s.at[l, xx], f_r.at[f], (PAIR * a + xx, l)).start()

    def layer(i, carry):
        l = layers - 1 - i
        ordered = planes == 4 and groups == 4
        upper = lax.div(a, 2)
        near = a + upper * (3 - 2 * a)
        relays = (a == 1) | (a == 2)

        def nearest(k):
            lower = lax.rem(near + k, 2) if k < 2 else k
            return lower + upper * (3 - 2 * lower)

        def pass_layer(m):
            @pl.when(relays)
            def _():
                take(m, nearest(3))

        def next_own(m):
            @pl.when(m > 0)
            def _():
                z_own(m - 1)

        if ordered:

            @pl.when((i == 1) | (i > 2))
            def _():
                pass_layer(l)
                next_own(l)

        for xx in range(PAIR):
            drain(act.at[l, xx, pl.ds(0, 3)], q_r.at[xx * sections + l])

        @pl.when(i == 0)
        def _():
            drain(og.at[0], cot_r.at[0])
            drain(og.at[0], cot_r.at[1])

        def attention(n, carry):
            xx, m = lax.div(n, micro), lax.rem(n, micro)
            for h in range(heads):
                at = pl.ds(h * HEAD_DIM, HEAD_DIM)
                q, k, v = (act[l, xx, t, m, :, at] for t in range(3))
                g = og[xx, m, :, at]
                scores = jnp.where(causal, dot(q, k, NT) * scale, -1e30)
                grown = jnp.exp(scores - jnp.max(scores, axis=-1, keepdims=True))
                attend = grown / jnp.sum(grown, axis=-1, keepdims=True)
                attend_grad = dot(g, v, NT)
                value_grad = dot(attend.astype(BF16), g, TN)
                row_total = jnp.sum(attend * attend_grad, axis=-1, keepdims=True)
                score_grad = (attend * (attend_grad - row_total) * scale).astype(BF16)
                ab[n, :, at] = dot(score_grad, k, NN).astype(BF16)
                ab[n, :, pl.ds(hw + h * HEAD_DIM, HEAD_DIM)] = dot(score_grad, q, TN).astype(BF16)
                ab[n, :, pl.ds(2 * hw + h * HEAD_DIM, HEAD_DIM)] = value_grad.astype(BF16)
            return carry

        lax.fori_loop(0, seqs, attention, 0, unroll=2)

        def flat(value):
            return value.reshape(-1, value.shape[-1])

        if ordered:

            @pl.when(i == 0)
            def _():
                pass_layer(l)

        drain(ad.at[l], ad_r.at[l])
        both[0, :rank] = (adapter_scale * dot(ad[l, 2 * rank : 3 * rank], flat(ab[:, :, :hw]), NT)).astype(BF16)
        both[0, rank:] = (adapter_scale * dot(ad[l, 3 * rank :], flat(ab[:, :, 2 * hw :]), NT)).astype(BF16)
        partner = device(flip(f, 1, cols))

        @pl.when(c == 1)
        def _():
            remote(both.at[0], pair_r, lp_s.at[0], lp_r.at[0], partner).start()

        down = ad[l, : 2 * rank]

        def normalise_all():
            for xx in range(PAIR):
                j = xx * sections + l
                drain(act.at[l, xx, 3], h_r.at[j])

                @pl.when(j != f)
                def _():
                    drain(st.at[j], st_r.at[j])

            drain(gn.at[l], gn_r.at[l])

            def normalise(n, carry):
                xx, m = lax.div(n, micro), lax.rem(n, micro)
                inverse = to_column(st[xx * sections + l, pl.ds(m, 1), :])
                nrm[n] = (act[l, xx, 3, m].astype(F32) * inverse * gn[l]).astype(BF16)
                return carry

            lax.fori_loop(0, seqs, normalise, 0, unroll=2)
            both[1] = dot(down, flat(nrm[...]), NT).astype(BF16)

            @pl.when(c == 0)
            def _():
                remote(both.at[1], pair_r, lp_s.at[0], lp_r.at[0], partner).start()

        def over_pair():
            drain(pair_r, lp_r.at[0])
            pair_t[...] = (both[c].astype(F32) + pair_r[...].astype(F32)).astype(BF16)
            for k in range(1, chips):
                target = device(2 * flip(chip, k, chips) + c)
                remote(pair_t, chip_r.at[chip], lx_s.at[k], lx_r.at[chip], target).start()

        def over_chips():
            total = pair_t[...].astype(F32)
            for k in range(1, chips):
                drain(chip_r.at[flip(chip, k, chips)], lx_r.at[flip(chip, k, chips)])
            for k in range(1, chips):
                total = total + chip_r[flip(chip, k, chips)].astype(F32)
            lowt[c] = total.astype(BF16)
            remote(lowt.at[c], lowt.at[c], lt_s.at[0], lt_r.at[0], partner).start()

        def group(t):
            if spread == block:
                w = wbuf.at[l, t]
            else:
                w = wbuf.at[l, pl.ds(t * (spread // block), spread // block)]

            def half(xx):
                tokens = flat(ab[pl.ds(xx * micro, micro)])
                return dot(tokens, flat(w[...]), NT).reshape(micro, seq, spread)

            cs[t] = half(1 - c).astype(BF16)
            to_partner = remote(cs.at[t], crecv.at[t], d_s.at[t], d_r.at[t], partner)
            to_partner.start()
            ctmp[...] = half(c)
            to_partner.wait_recv()
            total = ctmp[...] + crecv[t].astype(F32)
            core, u = lax.div(t, heads), lax.rem(t, heads)
            for i in range(chips):
                piece = total[:, :, i * HEAD_DIM : (i + 1) * HEAD_DIM].astype(BF16)
                target = 2 * i + core

                @pl.when(target == f)
                def _():
                    xrecv[u, chip, c] = piece

                @pl.when(target != f)
                def _():
                    xs[t, i] = piece
                    remote(
                        xs.at[t, i], xrecv.at[u, chip, c], x_s.at[t, i], x_r.at[u, chip, c], device(target)
                    ).start()

        def send_late():
            @pl.when(jnp.logical_not(early))
            def _():
                spread_out(weights, w_s, w_r)

        def gradients():
            drain(lowt.at[1 - c], lt_r.at[0])
            gr[l, a, : 2 * rank] = dot(lowt[0], flat(nrm[...]), NN).astype(BF16)
            gr[l, a, 2 * rank : 3 * rank] = (adapter_scale * dot(lowt[1, :rank], flat(ab[:, :, :hw]), NN)).astype(BF16)
            gr[l, a, 3 * rank :] = (adapter_scale * dot(lowt[1, rank:], flat(ab[:, :, 2 * hw :]), NN)).astype(BF16)
            for k in range(1, planes):
                there = (PAIR * lax.rem(a + k, planes) + x, s)
                remote(gr.at[l, a], gr.at[l, a], g_s.at[l, k], g_r.at[l, a], there).start()
            sc[...] = dot(lowt[0], down, TN).reshape(seqs, seq, hw)

        if ordered:
            pl.when(i > 1)(normalise_all)
            for k in range(4):
                t = nearest(k)
                if k == 1 or k == 2:
                    take(l, t)
                if k == 3:

                    pl.when(i == 0)(functools.partial(next_own, l))
                    pl.when(i < 2)(normalise_all)
                    pl.when((i < 2) & (c == 1))(over_pair)

                    @pl.when(jnp.logical_not(relays))
                    def _():
                        take(l, t)

                group(t)
                if k == 0:
                    pl.when((i > 1) | (c == 0))(over_pair)
                    pl.when(i == 0)(send_late)
        else:
            for d in range(1, planes):
                for b in (a - d, a + d):

                    @pl.when((b >= 0) & (b < planes))
                    def _():
                        take(l, b)

            pl.when(i == 0)(send_late)
            next_own(l)
            normalise_all()
            over_pair()
            for t in range(groups):
                group(jnp.int32(t))
        over_chips()
        gradients()
        if ordered:

            @pl.when((i == 1) & (l > 0))
            def _():
                pass_layer(l - 1)
                next_own(l - 1)

        pl.when(l == 0)(functools.partial(finish_grads, 0))

        for u in range(heads):
            for j in range(chips):
                for cc in range(2):

                    @pl.when((j != chip) | (cc != c))
                    def _():
                        drain(xrecv.at[u, j, cc], x_r.at[u, j, cc])

        def gather_up(n, carry):
            xx, m = lax.div(n, micro), lax.rem(n, micro)
            sums = []
            for u in range(heads):
                value = sc[n, :, u * HEAD_DIM : (u + 1) * HEAD_DIM]
                for j in range(chips):
                    value = value + xrecv[u, j, xx, m].astype(F32)
                value = gn[l, :, u * HEAD_DIM : (u + 1) * HEAD_DIM] * value
                sc[n, :, u * HEAD_DIM : (u + 1) * HEAD_DIM] = value
                sums.append(act[l, xx, 3, m, :, u * HEAD_DIM : (u + 1) * HEAD_DIM].astype(F32) * value)
            rs_own[pl.ds(n, 1), :] = to_row(jnp.sum(sum(sums), axis=-1, keepdims=True))
            return carry

        lax.fori_loop(0, seqs, gather_up, 0, unroll=2)
        for k, j in enumerate(others):
            remote(rs_own, rsr.at[f], rs_s.at[k], rs_r.at[f], device(j)).start()

        @pl.when(i == 0)
        def _():
            @pl.when(jnp.logical_not(early))
            def _():
                spread_out(lambda j: saved(j, (0, 1, 2)), q_s, q_r)
                spread_out(inputs, h_s, h_r)

        for j in others:
            drain(rsr.at[j], rs_r.at[j])
        correction = rs_own[...]
        for j in others:
            correction = correction + rsr[j]
        crow[...] = correction * (1.0 / features)

        @pl.when(i > 0)
        def _():
            for xx in range(PAIR):
                drain(og.at[xx], o_s.at[xx])

        def settle(n, carry):
            xx, m = lax.div(n, micro), lax.rem(n, micro)
            inverse = to_column(st[xx * sections + l, pl.ds(m, 1), :])
            corrected = to_column(crow[pl.ds(n, 1), :])
            hidden = act[l, xx, 3, m].astype(F32)
            og[xx, m] = (
                og[xx, m].astype(F32) + inverse * sc[n] - hidden * (inverse * inverse * inverse * corrected)
            ).astype(BF16)
            return carry

        lax.fori_loop(0, seqs, settle, 0, unroll=2)

        for xx in range(PAIR):
            mine = (x == xx) & (s == l)
            for dst, at in wide(f, out_ig.at[0, :, 0]):
                src = og.at[xx, :, :, at]

                @pl.when(mine)
                def _():
                    pltpu.make_async_copy(src, dst, o_s.at[xx]).start()

                @pl.when(jnp.logical_not(mine))
                def _():
                    remote(src, dst, o_s.at[xx], o_r.at[f], (PAIR * a + xx, l)).start()

        @pl.when(i > 0)
        def _():
            finish_grads(l + 1)

        for k in range(cols - 1):
            drain(rs_own, rs_s.at[k])
        drain(both.at[0], lp_s.at[0])
        drain(lowt.at[0], lt_s.at[0])
        for k in range(1, chips):
            drain(pair_t, lx_s.at[k])
        for t in range(groups):
            drain(cs.at[t], d_s.at[t])
            for j in range(chips):

                @pl.when(2 * j + t // heads != f)
                def _():
                    drain(xs.at[t, j], x_s.at[t, j])

        return carry

    lax.fori_loop(0, layers, layer, 0)

    for xx in range(PAIR):
        drain(og.at[xx], o_s.at[xx])
    for j in others:
        drain(og.at[0], o_r.at[j])
        drain(gf.at[0], f_r.at[j])
    for k in range(1, sections):
        drain(ad.at[0], ad_s.at[k])
        drain(gn.at[0], gn_s.at[k])
    drain(og.at[0], cot_s.at[0])
    for k in range(cols - 1):
        drain(wbuf.at[0, 0, pl.ds(0, rows_w), :], w_s.at[k])
        drain(act.at[0, 0, pl.ds(0, 3)], q_s.at[k])
        drain(act.at[0, 0, 3], h_s.at[k])
        drain(st_own, st_s.at[k])

    def sent(l, carry):
        for i, d in enumerate((2, -2, 1, -1)):
            if abs(d) >= planes:
                continue

            @pl.when((a + d >= 0) & (a + d < planes))
            def _():
                drain(wbuf.at[l, a], z_s.at[l, i])

        for d in range(2, planes):
            for b in (a - d, a + d):

                @pl.when((b >= 0) & (b < planes))
                def _():
                    passed_on(l, b, lambda copy: copy.wait_send())

        for k in range(1, planes):
            drain(gr.at[l, a], g_s.at[l, k])
        for xx in range(PAIR):
            drain(gf.at[l], f_s.at[l, xx])
        return carry

    lax.fori_loop(0, layers, sent, 0)


def on_device(n_dp, layers, *args):
    hidden, cot, w, down = args[0], args[4], args[6], args[9]
    micro, seq, features = cot.shape[0], cot.shape[2], cot.shape[3]
    batch = cot.shape[1] * n_dp
    rank, rows_w = down.shape[1], w.shape[1]
    planes, cols = n_dp // PAIR, PAIR * layers
    chips, hw, seqs = cols // 2, features // cols, PAIR * micro
    heads = hw // HEAD_DIM
    groups, spread = 2 * heads, chips * HEAD_DIM
    rows = seqs * seq
    pad = -(-micro // 8) * 8
    pads = -(-seqs // 8) * 8
    dma = pltpu.SemaphoreType.DMA
    vm = pltpu.VMEM
    scratch = [
        vm((layers, planes, PAIR * rows_w, 3 * hw), BF16),
        vm((layers, PAIR, 4, micro, seq, hw), BF16),
        vm((micro, seq, features), BF16),
        vm((PAIR, micro, seq, hw), BF16),
        vm((seqs, seq, 3 * hw), BF16),
        vm((seqs, seq, hw), BF16),
        vm((layers, 4 * rank, hw), BF16),
        vm((layers, 1, hw), F32),
        vm((cols, pad, 128), F32),
        vm((pad, 128), F32),
        vm((2, 2 * rank, rows), BF16),
        vm((2 * rank, rows), BF16),
        vm((2 * rank, rows), BF16),
        vm((chips, 2 * rank, rows), BF16),
        vm((2, 2 * rank, rows), BF16),
        vm((groups, micro, seq, spread), BF16),
        vm((groups, micro, seq, spread), BF16),
        vm((micro, seq, spread), F32),
        vm((groups, chips, micro, seq, HEAD_DIM), BF16),
        vm((heads, chips, 2, micro, seq, HEAD_DIM), BF16),
        vm((seqs, seq, hw), F32),
        vm((pads, 128), F32),
        vm((cols, pads, 128), F32),
        vm((pads, 128), F32),
        vm((layers, planes, 4 * rank, hw), BF16),
        vm((layers, 4 * rank, hw), F32),
    ]
    semaphores = [
        dma((cols,)), dma((cols,)), dma((cols,)), dma((cols,)), dma((cols,)), dma((cols,)),
        dma((layers,)), dma((layers,)), dma((layers,)), dma((layers,)), dma((1,)), dma((2,)), dma,
        dma((cols,)), dma((cols,)),
        dma((layers, 4)), dma((layers, planes)), dma((layers, planes)),
        dma((1,)), dma((1,)), dma((chips,)), dma((chips,)), dma((1,)), dma((1,)), dma((groups,)), dma((groups,)),
        dma((groups, chips)), dma((heads, chips, 2)),
        dma((cols,)), dma((cols,)), dma((PAIR,)), dma((cols,)),
        dma((layers, planes)), dma((layers, planes)), dma((layers, PAIR)), dma((cols,)),
    ]
    total_scale = (micro * batch * seq) ** (-0.5)
    any_space = pl.BlockSpec(memory_space=pl.ANY)
    input_grad, grads = pl.pallas_call(
        functools.partial(kernel, n_dp, layers, micro, seq, features, rank, rows_w, total_scale),
        out_shape=(
            jax.ShapeDtypeStruct(hidden.shape, BF16),
            jax.ShapeDtypeStruct((4 * rank, features), F32),
        ),
        in_specs=[any_space] * len(args),
        out_specs=(any_space, any_space),
        scratch_shapes=scratch + semaphores,
        compiler_params=pltpu.CompilerParams(
            collective_id=0, has_side_effects=True, vmem_limit_bytes=60 * 1024 * 1024
        ),
        name="section_backward",
    )(*args)
    return (
        input_grad,
        grads[None, :rank],
        grads[None, 2 * rank : 3 * rank],
        grads[None, rank : 2 * rank],
        grads[None, 3 * rank :],
    )


def solution(mesh):
    rows = P("section", None, "dp", None, None)
    cut = P("section", "dp", None)
    small = P("section", None, None)
    return jax.shard_map(
        functools.partial(on_device, mesh.shape["dp"], mesh.shape["section"]),
        mesh=mesh,
        in_specs=(rows,) * 4 + (P(None, "dp", None, None), P("section", None)) + (cut,) * 3 + (small,) * 4,
        out_specs=(rows,) + (small,) * 4,
        check_vma=False,
    )
```

```python
import functools

import jax
import jax.numpy as jnp
from jax import lax
from jax.experimental import pallas as pl
from jax.experimental.pallas import tpu as pltpu
from jax.sharding import PartitionSpec as P

HEAD_DIM = 128
adapter_scale = 2.0
norm_eps = 1e-05
NN = (((1,), (0,)), ((), ()))
NT = (((1,), (1,)), ((), ()))
TN = (((0,), (0,)), ((), ()))
F32 = jnp.float32
BF16 = jnp.bfloat16
MESH = pl.DeviceIdType.MESH
PAIR = 2


def dot(a, b, dims):
    return lax.dot_general(a, b, dims, preferred_element_type=F32)


def drain(ref, sem):
    pltpu.make_async_copy(ref, ref, sem).wait()


def remote(src, dst, send, recv, device):
    return pltpu.make_async_remote_copy(
        src_ref=src, dst_ref=dst, send_sem=send, recv_sem=recv, device_id=device, device_id_type=MESH
    )


def flip(value, k, size):
    if size & (size - 1):
        return lax.rem(value + k, size)
    out, bit = 0, 1
    while bit < size:
        out = out + bit * lax.rem(lax.div(value, bit) + (k // bit) % 2, 2)
        bit *= 2
    return out


def kernel(
    n_dp, layers, micro, seq, features, rank, rows_w, total_scale,
    hid, que, key, val, cot, gain, wq, wk, wv, dq, uq, dv, uv,
    out_ig, out_g,
    wbuf, act, hown, og, ab, nrm, ad, gn, st, st_own, both, pair_r, pair_t, chip_r, lowt,
    cs, crecv, ctmp, xs, xrecv, sc, rs_own, rsr, crow, gr, gf,
    w_s, w_r, q_s, q_r, h_s, h_r, ad_s, ad_r, gn_s, gn_r, cot_s, cot_r, hown_sem, st_s, st_r,
    z_s, z_r, rel_s, lp_s, lp_r, lx_s, lx_r, lt_s, lt_r, d_s, d_r, x_s, x_r, rs_s, rs_r, o_s, o_r, g_s, g_r, f_s, f_r,
):
    sections = layers
    planes = n_dp // PAIR
    cols = PAIR * sections
    chips = cols // 2
    hw = features // cols
    heads = hw // HEAD_DIM
    seqs = PAIR * micro
    block = PAIR * rows_w
    groups = 2 * heads
    spread = chips * HEAD_DIM
    dp, s = lax.axis_index("dp"), lax.axis_index("section")
    a, x = lax.div(dp, PAIR), lax.rem(dp, PAIR)
    f = x * sections + s
    c = lax.rem(f, 2)
    chip = lax.div(f, 2)

    def device(j):
        return (PAIR * a + lax.div(j, sections), lax.rem(j, sections))

    others = [flip(f, k, cols) for k in range(1, cols)]

    def wide(j, ref):
        for u in range(heads):
            at = ((lax.rem(j, 2) * heads + u) * chips + lax.div(j, 2)) * HEAD_DIM
            yield ref.at[..., pl.ds(pl.multiple_of(at, HEAD_DIM), HEAD_DIM)], pl.ds(u * HEAD_DIM, HEAD_DIM)

    barrier = pltpu.get_barrier_semaphore()
    for j in others:
        pl.semaphore_signal(barrier, inc=1, device_id=device(j), device_id_type=MESH)
    for k in range(1, planes):
        pl.semaphore_signal(
            barrier, inc=1, device_id=(PAIR * lax.rem(a + k, planes) + x, s), device_id_type=MESH
        )
    pl.semaphore_wait(barrier, cols - 1 + planes - 1)

    own_hidden = pltpu.make_async_copy(hid.at[0, :, 0], hown, hown_sem)
    own_hidden.start()
    for k in range(sections):
        s2 = s if k == 0 else flip(s, k, sections)
        j = x * sections + s2
        for i, ref in enumerate((dq, dv, uq, uv)):
            for src, at in wide(j, ref.at[0]):
                dst = ad.at[s, pl.ds(i * rank, rank), at]
                if k == 0:
                    pltpu.make_async_copy(src, dst, ad_r.at[s]).start()
                else:
                    remote(src, dst, ad_s.at[k], ad_r.at[s], (dp, s2)).start()
        for src, at in wide(j, gain):
            dst = gn.at[s, :, at]
            if k == 0:
                pltpu.make_async_copy(src, dst, gn_r.at[s]).start()
            else:
                remote(src, dst, gn_s.at[k], gn_r.at[s], (dp, s2)).start()
    mirror = (PAIR * a + 1 - x, s)
    for src, at in wide((1 - x) * sections + s, cot.at[:, 0]):
        remote(src, og.at[x, :, :, at], cot_s.at[0], cot_r.at[0], mirror).start()
    for src, at in wide(f, cot.at[:, 0]):
        pltpu.make_async_copy(src, og.at[x, :, :, at], cot_r.at[1]).start()

    def weights(j):
        for i, ref in enumerate((wq, wk, wv)):
            for u, (src, at) in enumerate(wide(j, ref.at[0])):
                yield src, wbuf.at[s, a, pl.ds(x * rows_w, rows_w), pl.ds(i * hw + u * HEAD_DIM, HEAD_DIM)]

    def saved(j, which=(0, 1, 2)):
        for i in which:
            for src, at in wide(j, (que, key, val)[i].at[0, :, 0]):
                yield src, act.at[s, x, i, :, :, at]

    def inputs(j):
        for src, at in wide(j, hid.at[0, :, 0]):
            yield src, act.at[s, x, 3, :, :, at]

    for group, recv in ((weights, w_r), (saved, q_r), (inputs, h_r)):
        for src, dst in group(f):
            pltpu.make_async_copy(src, dst, recv.at[f]).start()

    def spread_out(group, send, recv):
        for k, j in enumerate(others):
            for src, dst in group(j):
                remote(src, dst, send.at[k], recv.at[f], device(j)).start()

    early = lax.rem(layers - 1 - s, 2) == 0

    @pl.when(early)
    def _():
        spread_out(weights, w_s, w_r)
        spread_out(saved, q_s, q_r)
        spread_out(inputs, h_s, h_r)

    def z_half(l, xx):
        part = wbuf.at[l, a, pl.ds(xx * rows_w, rows_w), :]
        drain(part, w_r.at[xx * sections + l])
        for i, d in enumerate((2, -2, 1, -1)):
            if abs(d) >= planes:
                continue

            @pl.when((a + d >= 0) & (a + d < planes))
            def _():
                remote(part, part, z_s.at[l, i], z_r.at[l, a], (PAIR * (a + d) + x, s)).start()

    z_half(s, x)

    def z_own(l):
        for xx in range(PAIR):

            @pl.when((l != s) | (xx != x))
            def _():
                z_half(l, xx)

    eye = lax.broadcasted_iota(jnp.int32, (seq, 128), 0) == lax.broadcasted_iota(jnp.int32, (seq, 128), 1)

    def to_row(column):
        return jnp.sum(jnp.where(eye, column, 0.0), axis=0, keepdims=True)

    def to_column(row):
        return jnp.sum(jnp.where(eye, row, 0.0), axis=1, keepdims=True)

    own_hidden.wait()

    def inverse_of(m, carry):
        floated = hown[m].astype(F32)
        inverse = lax.rsqrt(jnp.mean(floated * floated, axis=-1, keepdims=True) + norm_eps)
        st_own[pl.ds(m, 1), :] = to_row(inverse)
        return carry

    lax.fori_loop(0, micro, inverse_of, 0)
    st[f] = st_own[...]
    for k, j in enumerate(others):
        remote(st_own, st.at[f], st_s.at[k], st_r.at[f], device(j)).start()

    def passed_on(l, b, todo):
        for direction in (1, -1):

            @pl.when(((a - b) * direction >= 2) & (a + direction >= 0) & (a + direction < planes))
            def _():
                todo(
                    remote(
                        wbuf.at[l, b], wbuf.at[l, b], rel_s.at[l, b], z_r.at[l, b],
                        (PAIR * (a + direction) + x, s),
                    )
                )

    def take(l, b):
        drain(wbuf.at[l, b], z_r.at[l, b])
        passed_on(l, b, lambda copy: copy.start())

    scale = HEAD_DIM ** (-0.5)
    causal = lax.broadcasted_iota(jnp.int32, (seq, seq), 1) <= lax.broadcasted_iota(jnp.int32, (seq, seq), 0)
    z_own(layers - 1)

    def finish_grads(l):
        for k in range(1, planes):
            b = lax.rem(a + k, planes)
            drain(gr.at[l, b], g_r.at[l, b])
        total = gr[l, 0].astype(F32)
        for b in range(1, planes):
            total = total + gr[l, b].astype(F32)
        gf[l] = total * total_scale
        for xx in range(PAIR):
            mine = (x == xx) & (s == l)
            for dst, at in wide(f, out_g):

                @pl.when(mine)
                def _():
                    pltpu.make_async_copy(gf.at[l, :, at], dst, f_s.at[l, xx]).start()

                @pl.when(jnp.logical_not(mine))
                def _():
                    remote(gf.at[l, :, at], dst, f_s.at[l, xx], f_r.at[f], (PAIR * a + xx, l)).start()

    def layer(i, carry):
        l = layers - 1 - i
        ordered = planes == 4 and groups == 4
        upper = lax.div(a, 2)
        near = a + upper * (3 - 2 * a)
        relays = (a == 1) | (a == 2)

        def nearest(k):
            lower = lax.rem(near + k, 2) if k < 2 else k
            return lower + upper * (3 - 2 * lower)

        def pass_layer(m):
            @pl.when(relays)
            def _():
                take(m, nearest(3))

        def next_own(m):
            @pl.when(m > 0)
            def _():
                z_own(m - 1)

        if ordered:

            @pl.when((i == 1) | (i > 2))
            def _():
                pass_layer(l)
                next_own(l)

        for xx in range(PAIR):
            drain(act.at[l, xx, pl.ds(0, 3)], q_r.at[xx * sections + l])

        @pl.when(i == 0)
        def _():
            drain(og.at[0], cot_r.at[0])
            drain(og.at[0], cot_r.at[1])

        def attention(n, carry):
            xx, m = lax.div(n, micro), lax.rem(n, micro)
            for h in range(heads):
                at = pl.ds(h * HEAD_DIM, HEAD_DIM)
                q, k, v = (act[l, xx, t, m, :, at] for t in range(3))
                g = og[xx, m, :, at]
                scores = jnp.where(causal, dot(q, k, NT) * scale, -1e30)
                grown = jnp.exp(scores - jnp.max(scores, axis=-1, keepdims=True))
                attend = grown / jnp.sum(grown, axis=-1, keepdims=True)
                attend_grad = dot(g, v, NT)
                value_grad = dot(attend.astype(BF16), g, TN)
                row_total = jnp.sum(attend * attend_grad, axis=-1, keepdims=True)
                score_grad = (attend * (attend_grad - row_total) * scale).astype(BF16)
                ab[n, :, at] = dot(score_grad, k, NN).astype(BF16)
                ab[n, :, pl.ds(hw + h * HEAD_DIM, HEAD_DIM)] = dot(score_grad, q, TN).astype(BF16)
                ab[n, :, pl.ds(2 * hw + h * HEAD_DIM, HEAD_DIM)] = value_grad.astype(BF16)
            return carry

        lax.fori_loop(0, seqs, attention, 0, unroll=2)

        def flat(value):
            return value.reshape(-1, value.shape[-1])

        if ordered:

            @pl.when(i == 0)
            def _():
                pass_layer(l)

        drain(ad.at[l], ad_r.at[l])
        both[0, :rank] = (adapter_scale * dot(ad[l, 2 * rank : 3 * rank], flat(ab[:, :, :hw]), NT)).astype(BF16)
        both[0, rank:] = (adapter_scale * dot(ad[l, 3 * rank :], flat(ab[:, :, 2 * hw :]), NT)).astype(BF16)
        partner = device(flip(f, 1, cols))

        @pl.when(c == 1)
        def _():
            remote(both.at[0], pair_r, lp_s.at[0], lp_r.at[0], partner).start()

        down = ad[l, : 2 * rank]

        def normalise_all():
            for xx in range(PAIR):
                j = xx * sections + l
                drain(act.at[l, xx, 3], h_r.at[j])

                @pl.when(j != f)
                def _():
                    drain(st.at[j], st_r.at[j])

            drain(gn.at[l], gn_r.at[l])

            def normalise(n, carry):
                xx, m = lax.div(n, micro), lax.rem(n, micro)
                inverse = to_column(st[xx * sections + l, pl.ds(m, 1), :])
                nrm[n] = (act[l, xx, 3, m].astype(F32) * inverse * gn[l]).astype(BF16)
                return carry

            lax.fori_loop(0, seqs, normalise, 0, unroll=4)
            both[1] = dot(down, flat(nrm[...]), NT).astype(BF16)

            @pl.when(c == 0)
            def _():
                remote(both.at[1], pair_r, lp_s.at[0], lp_r.at[0], partner).start()

        def over_pair():
            drain(pair_r, lp_r.at[0])
            pair_t[...] = (both[c].astype(F32) + pair_r[...].astype(F32)).astype(BF16)
            for k in range(1, chips):
                target = device(2 * flip(chip, k, chips) + c)
                remote(pair_t, chip_r.at[chip], lx_s.at[k], lx_r.at[chip], target).start()

        def over_chips():
            total = pair_t[...].astype(F32)
            for k in range(1, chips):
                drain(chip_r.at[flip(chip, k, chips)], lx_r.at[flip(chip, k, chips)])
            for k in range(1, chips):
                total = total + chip_r[flip(chip, k, chips)].astype(F32)
            lowt[c] = total.astype(BF16)
            remote(lowt.at[c], lowt.at[c], lt_s.at[0], lt_r.at[0], partner).start()

        def group(t):
            if spread == block:
                w = wbuf.at[l, t]
            else:
                w = wbuf.at[l, pl.ds(t * (spread // block), spread // block)]

            def half(xx):
                tokens = flat(ab[pl.ds(xx * micro, micro)])
                return dot(tokens, flat(w[...]), NT).reshape(micro, seq, spread)

            cs[t] = half(1 - c).astype(BF16)
            to_partner = remote(cs.at[t], crecv.at[t], d_s.at[t], d_r.at[t], partner)
            to_partner.start()
            ctmp[...] = half(c)
            to_partner.wait_recv()
            total = ctmp[...] + crecv[t].astype(F32)
            core, u = lax.div(t, heads), lax.rem(t, heads)
            for i in range(chips):
                piece = total[:, :, i * HEAD_DIM : (i + 1) * HEAD_DIM].astype(BF16)
                target = 2 * i + core

                @pl.when(target == f)
                def _():
                    xrecv[u, chip, c] = piece

                @pl.when(target != f)
                def _():
                    xs[t, i] = piece
                    remote(
                        xs.at[t, i], xrecv.at[u, chip, c], x_s.at[t, i], x_r.at[u, chip, c], device(target)
                    ).start()

        def send_late():
            @pl.when(jnp.logical_not(early))
            def _():
                spread_out(weights, w_s, w_r)

        def gradients():
            drain(lowt.at[1 - c], lt_r.at[0])
            gr[l, a, : 2 * rank] = dot(lowt[0], flat(nrm[...]), NN).astype(BF16)
            gr[l, a, 2 * rank : 3 * rank] = (adapter_scale * dot(lowt[1, :rank], flat(ab[:, :, :hw]), NN)).astype(BF16)
            gr[l, a, 3 * rank :] = (adapter_scale * dot(lowt[1, rank:], flat(ab[:, :, 2 * hw :]), NN)).astype(BF16)
            for k in range(1, planes):
                there = (PAIR * lax.rem(a + k, planes) + x, s)
                remote(gr.at[l, a], gr.at[l, a], g_s.at[l, k], g_r.at[l, a], there).start()
            sc[...] = dot(lowt[0], down, TN).reshape(seqs, seq, hw)

        if ordered:
            pl.when(i > 1)(normalise_all)
            for k in range(4):
                t = nearest(k)
                if k == 1 or k == 2:
                    take(l, t)
                if k == 3:

                    pl.when(i == 0)(functools.partial(next_own, l))
                    pl.when(i < 2)(normalise_all)
                    pl.when((i < 2) & (c == 1))(over_pair)

                    @pl.when(jnp.logical_not(relays))
                    def _():
                        take(l, t)

                group(t)
                if k == 0:
                    pl.when((i > 1) | (c == 0))(over_pair)
                    pl.when(i == 0)(send_late)
        else:
            for d in range(1, planes):
                for b in (a - d, a + d):

                    @pl.when((b >= 0) & (b < planes))
                    def _():
                        take(l, b)

            pl.when(i == 0)(send_late)
            next_own(l)
            normalise_all()
            over_pair()
            for t in range(groups):
                group(jnp.int32(t))
        over_chips()
        gradients()
        if ordered:

            @pl.when((i == 1) & (l > 0))
            def _():
                pass_layer(l - 1)
                next_own(l - 1)

        pl.when(l == 0)(functools.partial(finish_grads, 0))

        for u in range(heads):
            for j in range(chips):
                for cc in range(2):

                    @pl.when((j != chip) | (cc != c))
                    def _():
                        drain(xrecv.at[u, j, cc], x_r.at[u, j, cc])

        def gather_up(n, carry):
            xx, m = lax.div(n, micro), lax.rem(n, micro)
            sums = []
            for u in range(heads):
                value = sc[n, :, u * HEAD_DIM : (u + 1) * HEAD_DIM]
                for j in range(chips):
                    value = value + xrecv[u, j, xx, m].astype(F32)
                value = gn[l, :, u * HEAD_DIM : (u + 1) * HEAD_DIM] * value
                sc[n, :, u * HEAD_DIM : (u + 1) * HEAD_DIM] = value
                sums.append(act[l, xx, 3, m, :, u * HEAD_DIM : (u + 1) * HEAD_DIM].astype(F32) * value)
            rs_own[pl.ds(n, 1), :] = to_row(jnp.sum(sum(sums), axis=-1, keepdims=True))
            return carry

        lax.fori_loop(0, seqs, gather_up, 0, unroll=4)
        for k, j in enumerate(others):
            remote(rs_own, rsr.at[f], rs_s.at[k], rs_r.at[f], device(j)).start()

        @pl.when(i == 0)
        def _():
            @pl.when(jnp.logical_not(early))
            def _():
                spread_out(lambda j: saved(j, (0, 1, 2)), q_s, q_r)
                spread_out(inputs, h_s, h_r)

        for j in others:
            drain(rsr.at[j], rs_r.at[j])
        correction = rs_own[...]
        for j in others:
            correction = correction + rsr[j]
        crow[...] = correction * (1.0 / features)

        @pl.when(i > 0)
        def _():
            for xx in range(PAIR):
                drain(og.at[xx], o_s.at[xx])

        def settle(n, carry):
            xx, m = lax.div(n, micro), lax.rem(n, micro)
            inverse = to_column(st[xx * sections + l, pl.ds(m, 1), :])
            corrected = to_column(crow[pl.ds(n, 1), :])
            hidden = act[l, xx, 3, m].astype(F32)
            og[xx, m] = (
                og[xx, m].astype(F32) + inverse * sc[n] - hidden * (inverse * inverse * inverse * corrected)
            ).astype(BF16)
            return carry

        lax.fori_loop(0, seqs, settle, 0, unroll=4)

        for xx in range(PAIR):
            mine = (x == xx) & (s == l)
            for dst, at in wide(f, out_ig.at[0, :, 0]):
                src = og.at[xx, :, :, at]

                @pl.when(mine)
                def _():
                    pltpu.make_async_copy(src, dst, o_s.at[xx]).start()

                @pl.when(jnp.logical_not(mine))
                def _():
                    remote(src, dst, o_s.at[xx], o_r.at[f], (PAIR * a + xx, l)).start()

        @pl.when(i > 0)
        def _():
            finish_grads(l + 1)

        for k in range(cols - 1):
            drain(rs_own, rs_s.at[k])
        drain(both.at[0], lp_s.at[0])
        drain(lowt.at[0], lt_s.at[0])
        for k in range(1, chips):
            drain(pair_t, lx_s.at[k])
        for t in range(groups):
            drain(cs.at[t], d_s.at[t])
            for j in range(chips):

                @pl.when(2 * j + t // heads != f)
                def _():
                    drain(xs.at[t, j], x_s.at[t, j])

        return carry

    lax.fori_loop(0, layers, layer, 0)

    for xx in range(PAIR):
        drain(og.at[xx], o_s.at[xx])
    for j in others:
        drain(og.at[0], o_r.at[j])
        drain(gf.at[0], f_r.at[j])
    for k in range(1, sections):
        drain(ad.at[0], ad_s.at[k])
        drain(gn.at[0], gn_s.at[k])
    drain(og.at[0], cot_s.at[0])
    for k in range(cols - 1):
        drain(wbuf.at[0, 0, pl.ds(0, rows_w), :], w_s.at[k])
        drain(act.at[0, 0, pl.ds(0, 3)], q_s.at[k])
        drain(act.at[0, 0, 3], h_s.at[k])
        drain(st_own, st_s.at[k])

    def sent(l, carry):
        for i, d in enumerate((2, -2, 1, -1)):
            if abs(d) >= planes:
                continue

            @pl.when((a + d >= 0) & (a + d < planes))
            def _():
                drain(wbuf.at[l, a], z_s.at[l, i])

        for d in range(2, planes):
            for b in (a - d, a + d):

                @pl.when((b >= 0) & (b < planes))
                def _():
                    passed_on(l, b, lambda copy: copy.wait_send())

        for k in range(1, planes):
            drain(gr.at[l, a], g_s.at[l, k])
        for xx in range(PAIR):
            drain(gf.at[l], f_s.at[l, xx])
        return carry

    lax.fori_loop(0, layers, sent, 0)


def on_device(n_dp, layers, *args):
    hidden, cot, w, down = args[0], args[4], args[6], args[9]
    micro, seq, features = cot.shape[0], cot.shape[2], cot.shape[3]
    batch = cot.shape[1] * n_dp
    rank, rows_w = down.shape[1], w.shape[1]
    planes, cols = n_dp // PAIR, PAIR * layers
    chips, hw, seqs = cols // 2, features // cols, PAIR * micro
    heads = hw // HEAD_DIM
    groups, spread = 2 * heads, chips * HEAD_DIM
    rows = seqs * seq
    pad = -(-micro // 8) * 8
    pads = -(-seqs // 8) * 8
    dma = pltpu.SemaphoreType.DMA
    vm = pltpu.VMEM
    scratch = [
        vm((layers, planes, PAIR * rows_w, 3 * hw), BF16),
        vm((layers, PAIR, 4, micro, seq, hw), BF16),
        vm((micro, seq, features), BF16),
        vm((PAIR, micro, seq, hw), BF16),
        vm((seqs, seq, 3 * hw), BF16),
        vm((seqs, seq, hw), BF16),
        vm((layers, 4 * rank, hw), BF16),
        vm((layers, 1, hw), F32),
        vm((cols, pad, 128), F32),
        vm((pad, 128), F32),
        vm((2, 2 * rank, rows), BF16),
        vm((2 * rank, rows), BF16),
        vm((2 * rank, rows), BF16),
        vm((chips, 2 * rank, rows), BF16),
        vm((2, 2 * rank, rows), BF16),
        vm((groups, micro, seq, spread), BF16),
        vm((groups, micro, seq, spread), BF16),
        vm((micro, seq, spread), F32),
        vm((groups, chips, micro, seq, HEAD_DIM), BF16),
        vm((heads, chips, 2, micro, seq, HEAD_DIM), BF16),
        vm((seqs, seq, hw), F32),
        vm((pads, 128), F32),
        vm((cols, pads, 128), F32),
        vm((pads, 128), F32),
        vm((layers, planes, 4 * rank, hw), BF16),
        vm((layers, 4 * rank, hw), F32),
    ]
    semaphores = [
        dma((cols,)), dma((cols,)), dma((cols,)), dma((cols,)), dma((cols,)), dma((cols,)),
        dma((layers,)), dma((layers,)), dma((layers,)), dma((layers,)), dma((1,)), dma((2,)), dma,
        dma((cols,)), dma((cols,)),
        dma((layers, 4)), dma((layers, planes)), dma((layers, planes)),
        dma((1,)), dma((1,)), dma((chips,)), dma((chips,)), dma((1,)), dma((1,)), dma((groups,)), dma((groups,)),
        dma((groups, chips)), dma((heads, chips, 2)),
        dma((cols,)), dma((cols,)), dma((PAIR,)), dma((cols,)),
        dma((layers, planes)), dma((layers, planes)), dma((layers, PAIR)), dma((cols,)),
    ]
    total_scale = (micro * batch * seq) ** (-0.5)
    any_space = pl.BlockSpec(memory_space=pl.ANY)
    input_grad, grads = pl.pallas_call(
        functools.partial(kernel, n_dp, layers, micro, seq, features, rank, rows_w, total_scale),
        out_shape=(
            jax.ShapeDtypeStruct(hidden.shape, BF16),
            jax.ShapeDtypeStruct((4 * rank, features), F32),
        ),
        in_specs=[any_space] * len(args),
        out_specs=(any_space, any_space),
        scratch_shapes=scratch + semaphores,
        compiler_params=pltpu.CompilerParams(
            collective_id=0, has_side_effects=True, vmem_limit_bytes=60 * 1024 * 1024
        ),
        name="section_backward",
    )(*args)
    return (
        input_grad,
        grads[None, :rank],
        grads[None, 2 * rank : 3 * rank],
        grads[None, rank : 2 * rank],
        grads[None, 3 * rank :],
    )


def solution(mesh):
    rows = P("section", None, "dp", None, None)
    cut = P("section", "dp", None)
    small = P("section", None, None)
    return jax.shard_map(
        functools.partial(on_device, mesh.shape["dp"], mesh.shape["section"]),
        mesh=mesh,
        in_specs=(rows,) * 4 + (P(None, "dp", None, None), P("section", None)) + (cut,) * 3 + (small,) * 4,
        out_specs=(rows,) + (small,) * 4,
        check_vma=False,
    )
```
